32 devices in a mesh: groups: 2 (over y), blk: 4 (over z), ulysses: 2 (over x), cfg: 2 (over core).
Axes of the slice: x: 2, y: 2, z: 4, core: 2. Of those that a mesh axis runs over, the one named last changes fastest.
Arguments:
- img_tokens: bfloat16 [2, 2, 512, 2432], P('cfg', 'groups', ('blk', 'ulysses')), parts along dimension 1, may hold values from -72 to 72
- text_tokens: bfloat16 [2, 2, 48, 2432], P('cfg', 'groups', ('blk', 'ulysses')), parts along dimension 1, may hold values from -6 to 6
- text_lengths: int32 [2, 2], P('cfg', 'groups'), parts along dimension 1, may hold values from 12 to 48
- timestep: int32 [2], P('groups'), parts along dimension 0, may hold values from 0 to 999
- pooled: float32 [2, 2, 2432], P(None, 'groups'), parts along dimension 1, may hold values from -6 to 6
- time_weight: bfloat16 [256, 2432], replicated, may hold values from -0.375 to 0.375
- time_second: bfloat16 [2432, 2432], P(None, ('blk', 'ulysses', 'cfg')), may hold values from -0.125 to 0.125
- mod_weight: bfloat16 [2432, 24320], P(None, ('blk', 'ulysses', 'cfg')), may hold values from -0.125 to 0.125
- proj_weight: bfloat16 [5, 2432, 2048], P(None, None, ('ulysses', 'cfg')), may hold values from -0.125 to 0.125
- out_weight: bfloat16 [2048, 2432], P(('ulysses', 'cfg')), may hold values from -0.125 to 0.125
- expand_weight: bfloat16 [2432, 7168], P('blk', ('ulysses', 'cfg')), may hold values from -0.125 to 0.125
- reduce_weight: bfloat16 [7168, 2432], P(('ulysses', 'cfg'), 'blk'), may hold values from -0.0625 to 0.0625
- qk_gain: float32 [3, 64], replicated, may hold values from 0.5 to 10
- final_weight: bfloat16 [2432, 64], replicated, may hold values from -0.125 to 0.125
Outputs:
- guided: float32 [2, 16, 16, 128], P('groups', None, ('blk', 'ulysses', 'cfg')), parts along dimension 0
The draws below stay inside these ranges and needn't reach their ends.
There are 2 independent parts, one for each index of `groups`. The reference program is written for one: setup_inputs(seed, part) draws one part's arguments, and reference() takes and returns one part's arrays. A program takes and returns all parts, laid end to end along the dimension named above; an argument that names none is the same for every part. Nothing has to cross between parts.
All inputs are finite; a program needn't handle non-finite values.
Results may differ from the reference program's by a relative error of at most 0.011.
The reference program's roundings to bfloat16 on the way count: a program that leaves them out, or rounds other values in their place, can miss the bound.
Values may be sent and summed in bfloat16 or wider, within the bound.
A program may use at most 192 MiB of HBM per device.

```python
import math
import jax
import jax.numpy as jnp
from jax import lax

D = 2432
HEADS = 32
HD = 64
LAT = 16
FREQ = 256
FF = 7168
PROMPTS = 1
IMG_DEV = 64
INNER = 2048
PATCH_OUT = 64
IMG = 512
TXT = 48
N_ULYSSES = 2
N_CFG = 2


def draw_img_tokens(key, part):
    base_key, row_key, col_key = jax.random.split(jax.random.fold_in(key, 11), 3)
    full_shape = (2, PROMPTS, IMG, D)
    base_draw = jnp.clip(jax.random.normal(base_key, full_shape, jnp.float32), -4.0, 4.0)
    row_top = math.log(4.0)
    row_scale = jnp.exp(jax.random.uniform(row_key, (2, PROMPTS, IMG, 1), jnp.float32, 0.0, row_top))
    col_scale = jnp.exp(jax.random.uniform(col_key, (1, 1, 1, D), jnp.float32, math.log(0.5), math.log(2.0)))
    return (base_draw * row_scale * col_scale).astype(jnp.bfloat16)


def draw_qk_gain(key, part):
    gain_key = jax.random.fold_in(key, 23)
    low_end = math.log(0.5)
    high_end = math.log(2.0)
    return jnp.exp(jax.random.uniform(gain_key, (3, HD), jnp.float32, low_end, high_end))


def shard_levels(key, shape, cuts, smallest, largest):
    def one(position, blocks):
        heights = jax.random.uniform(jax.random.fold_in(jax.random.fold_in(key, 6), position), (blocks,), jnp.float32, smallest / len(cuts), largest / len(cuts))
        return jnp.repeat(jnp.exp(heights), shape[position] // blocks).reshape((-1,) + (1,) * (len(shape) - position - 1))

    level = one(*cuts[0])
    for cut in cuts[1:]:
        level = level * one(*cut)
    return level


def normal_values(stream_key, dims, deviation, bound, shards=(), kind=jnp.bfloat16):
    factor_of = shard_levels(stream_key, dims, shards, -0.22, 0.18) if shards else 1.0
    result = jax.random.normal(stream_key, dims, jnp.float32) * deviation * factor_of
    return jnp.minimum(jnp.maximum(result, -bound), bound).astype(kind)


def setup_inputs(seed: int = 0, part: int = 0) -> dict:
    key_list = jax.random.split(jax.random.key(seed), 15)
    part_keys = jax.random.split(jax.random.fold_in(key_list[14], part), 15)
    img_tokens = draw_img_tokens(jax.random.fold_in(jax.random.fold_in(key_list[14], part), 71), part)
    text_tokens = normal_values(part_keys[1], (2, PROMPTS, TXT, D), 1.0, 6.0, ((0, 2), (2, 8)))
    text_lengths = jax.random.randint(part_keys[2], (2, PROMPTS), TXT // 4, TXT + 1).astype(jnp.int32)
    timestep = jax.random.randint(part_keys[3], (PROMPTS,), 0, 1000).astype(jnp.int32)
    pooled = normal_values(part_keys[4], (2, PROMPTS, D), 1.0, 6.0, (), jnp.float32)
    time_weight = normal_values(key_list[5], (FREQ, D), FREQ ** -0.5, 0.375)
    time_second = normal_values(key_list[6], (D, D), D ** -0.5, 0.125, ((1, 16),))
    mod_weight = normal_values(key_list[7], (D, 10 * D), D ** -0.5, 0.125, ((1, 16),))
    proj_weight = normal_values(key_list[8], (5, D, INNER), D ** -0.5, 0.125, ((2, 4),))
    out_weight = normal_values(key_list[9], (INNER, D), INNER ** -0.5, 0.125, ((0, 4),))
    expand_weight = normal_values(key_list[10], (D, FF), D ** -0.5, 0.125, ((0, 4), (1, 4)))
    reduce_weight = normal_values(key_list[11], (FF, D), FF ** -0.5, 0.0625, ((0, 4), (1, 4)))
    qk_gain = draw_qk_gain(jax.random.fold_in(key_list[14], 71), part)
    final_weight = normal_values(key_list[13], (D, PATCH_OUT), D ** -0.5, 0.125)
    return {"img_tokens": img_tokens, "text_tokens": text_tokens, "text_lengths": text_lengths, "timestep": timestep, "pooled": pooled, "time_weight": time_weight, "time_second": time_second, "mod_weight": mod_weight, "proj_weight": proj_weight, "out_weight": out_weight, "expand_weight": expand_weight, "reduce_weight": reduce_weight, "qk_gain": qk_gain, "final_weight": final_weight}


GUIDANCE = 3.5
LN_EPS = 1e-06
RMS_EPS = 1e-06
NEG_FILL = -1e+30

def sinusoid(timestep, feature_count):
    half_width = feature_count // 2
    frequency = jnp.exp(-math.log(10000.0) * jnp.arange(half_width, dtype=jnp.float32) / half_width)
    angles = timestep.astype(jnp.float32)[:, None] * frequency[None, :]
    return jnp.concatenate([jnp.cos(angles), jnp.sin(angles)], axis=1)

def layer_norm(values):
    average = lax.optimization_barrier(jnp.mean(values, axis=-1, keepdims=True))
    centred = values - average
    variance = lax.optimization_barrier(jnp.mean(centred * centred, axis=-1, keepdims=True))
    return centred * lax.rsqrt(variance + LN_EPS)

def modulate(values, shift, scale):
    return (layer_norm(values.astype(jnp.float32)) * (1.0 + scale) + shift).astype(jnp.bfloat16)

def rms_heads(values, gain):
    head_size = gain.shape[0]
    shaped = values.reshape(values.shape[:-1] + (values.shape[-1] // head_size, head_size))
    inverse = lax.rsqrt(lax.optimization_barrier(jnp.mean(shaped * shaped, axis=-1, keepdims=True)) + RMS_EPS)
    return (shaped * inverse * gain).reshape(values.shape).astype(jnp.bfloat16)

def finish(img_proj, txt_proj, gain_rows):
    img_set = jnp.stack([rms_heads(img_proj[0], gain_rows[0]), rms_heads(img_proj[1], gain_rows[1]), img_proj[2].astype(jnp.bfloat16)])
    txt_set = jnp.stack([rms_heads(txt_proj[0], gain_rows[2]), txt_proj[1].astype(jnp.bfloat16)])
    return (img_set, txt_set)

def head_attention(query_head, key_head, value_head, usable):
    scores = jnp.dot(query_head, key_head.T, preferred_element_type=jnp.float32) * (1.0 / math.sqrt(query_head.shape[1]))
    scores = jnp.where(usable[None, :], scores, NEG_FILL)
    row_max = lax.optimization_barrier(jnp.max(scores, axis=1, keepdims=True))
    weights = jnp.where(usable[None, :], jnp.exp(scores - row_max), 0.0)
    row_total = lax.optimization_barrier(jnp.sum(weights, axis=1, keepdims=True))
    mixed = jnp.dot(weights.astype(jnp.bfloat16), value_head, preferred_element_type=jnp.float32) / row_total
    return mixed.astype(jnp.bfloat16)

def feed_forward(feed_input, expand_weight, reduce_weight):
    feed_hidden = jax.nn.gelu(jnp.dot(feed_input, expand_weight, preferred_element_type=jnp.float32), approximate=True).astype(jnp.bfloat16)
    group_count = N_ULYSSES * N_CFG
    group_width = reduce_weight.shape[0] // group_count
    feed_out = jnp.zeros((feed_input.shape[0], reduce_weight.shape[1]), jnp.float32)
    for group in range(group_count):
        term = jnp.dot(feed_hidden[:, group * group_width:(group + 1) * group_width], reduce_weight[group * group_width:(group + 1) * group_width], preferred_element_type=jnp.float32)
        term = lax.optimization_barrier(term.astype(jnp.bfloat16))
        feed_out = feed_out + term.astype(jnp.float32)
    return feed_out

def one_branch(image_rows, text_rows, length, mod_rows, proj_weight, out_weight, expand_weight, reduce_weight, qk_gain, final_weight):
    h_img = modulate(image_rows, mod_rows[0], mod_rows[1])
    h_txt = modulate(text_rows, mod_rows[4], mod_rows[3])
    img_proj = jnp.stack([jnp.dot(h_img, proj_weight[j], preferred_element_type=jnp.float32) for j in range(3)])
    txt_proj = jnp.stack([jnp.dot(h_txt, proj_weight[j], preferred_element_type=jnp.float32) for j in (3, 4)])
    img_set, txt_set = finish(img_proj, txt_proj, qk_gain)
    key_rows = jnp.concatenate([img_set[1], txt_set[0]], axis=0)
    value_rows = jnp.concatenate([img_set[2], txt_set[1]], axis=0)
    usable = jnp.concatenate([jnp.ones((IMG,), dtype=bool), jnp.arange(TXT, dtype=jnp.int32) < length])
    query_stack = img_set[0].reshape(IMG, HEADS, HD).transpose(1, 0, 2)
    key_stack = key_rows.reshape(IMG + TXT, HEADS, HD).transpose(1, 0, 2)
    value_stack = value_rows.reshape(IMG + TXT, HEADS, HD).transpose(1, 0, 2)

    def per_head(triple):
        return head_attention(triple[0], triple[1], triple[2], usable)
    mixed = lax.map(per_head, (query_stack, key_stack, value_stack))
    mixed = mixed.transpose(1, 0, 2).reshape(IMG, INNER)
    grouped = mixed.reshape(IMG, N_ULYSSES, INNER // N_ULYSSES).astype(jnp.float32)
    weight_groups = out_weight.reshape(N_ULYSSES, INNER // N_ULYSSES, D).astype(jnp.float32)
    group_terms = jnp.einsum('igc,gcd->gid', grouped, weight_groups, precision=lax.Precision.HIGHEST)
    group_terms = lax.optimization_barrier(group_terms.astype(jnp.bfloat16))
    attended = lax.optimization_barrier(jnp.sum(group_terms.astype(jnp.float32), axis=0))
    residual = image_rows.astype(jnp.float32) + mod_rows[2] * attended
    feed_input = modulate(residual, mod_rows[7], mod_rows[8])
    feed_out = feed_forward(feed_input, expand_weight, reduce_weight)
    second_residual = residual + mod_rows[9] * feed_out
    final_rows = modulate(second_residual, mod_rows[6], mod_rows[5])
    noise = jnp.dot(final_rows, final_weight, preferred_element_type=jnp.float32)
    noise = noise.reshape(IMG // IMG_DEV, IMG_DEV, 2, 2, LAT).transpose(4, 0, 2, 1, 3)
    return noise.reshape(LAT, 2 * IMG // IMG_DEV, 2 * IMG_DEV)

def reference(img_tokens, text_tokens, text_lengths, timestep, pooled, time_weight, time_second, mod_weight, proj_weight, out_weight, expand_weight, reduce_weight, qk_gain, final_weight):
    sinusoid_rows = sinusoid(timestep, time_weight.shape[0]).astype(jnp.bfloat16)
    time_hidden = jax.nn.silu(jnp.dot(sinusoid_rows, time_weight, preferred_element_type=jnp.float32)).astype(jnp.bfloat16)
    time_embed = jnp.dot(time_hidden, time_second, preferred_element_type=jnp.float32)
    acted = jax.nn.silu(time_embed[None] + pooled).astype(jnp.bfloat16)
    modulation = jnp.dot(acted.reshape(2 * PROMPTS, D), mod_weight, preferred_element_type=jnp.float32)
    modulation = modulation.reshape(2, PROMPTS, 10, D)
    results = []
    for prompt in range(PROMPTS):
        noises = []
        for branch in range(2):
            noises.append(one_branch(img_tokens[branch, prompt], text_tokens[branch, prompt], text_lengths[branch, prompt], modulation[branch, prompt], proj_weight, out_weight, expand_weight, reduce_weight, qk_gain, final_weight))
        noise_cond = noises[0]
        noise_uncond = noises[1]
        results.append(noise_uncond + GUIDANCE * (noise_cond - noise_uncond))
    return jnp.stack(results)
```

```python
import functools
import math

import jax
import jax.numpy as jnp
from jax import lax
from jax.experimental import pallas as pl
from jax.experimental.pallas import tpu as pltpu
from jax.sharding import PartitionSpec as P


GUIDANCE = 3.5
LN_EPS = 1e-06
RMS_EPS = 1e-06
NEG_FILL = -1e30
MESH = pl.DeviceIdType.MESH


def from_partner(value, axis, stride):
    mask = 2**stride
    pairs = [(source, source ^ mask) for source in range(lax.axis_size(axis))]
    return lax.ppermute(value, axis, pairs)


def sinusoid(timestep, feature_count):
    half_width = feature_count // 2
    frequency = jnp.exp(-math.log(10000.0) * jnp.arange(half_width, dtype=jnp.float32) / half_width)
    angles = timestep.astype(jnp.float32)[:, None] * frequency[None, :]
    return jnp.concatenate([jnp.cos(angles), jnp.sin(angles)], axis=1)


def layer_norm(values):
    average = jnp.mean(values, axis=-1, keepdims=True)
    centred = values - average
    variance = jnp.mean(centred * centred, axis=-1, keepdims=True)
    return centred * lax.rsqrt(variance + LN_EPS)


def modulate(values, shift, scale):
    return (layer_norm(values.astype(jnp.float32)) * (1.0 + scale) + shift).astype(jnp.bfloat16)


def reduce_kernel(axes, x_ref, o_ref, got, mine, core_s, core_r, far_s, far_r):
    count = count_of(axes)
    me = flat_position(axes)
    core = lax.axis_index("cfg")
    partner = {"cfg": 1 - core}
    inner = x_ref.shape[2]
    barrier = pltpu.get_barrier_semaphore()
    pl.semaphore_signal(barrier, inc=1, device_id=partner, device_id_type=MESH)

    def target(step):
        return lax.rem(me + step, count)

    def greet(step, carry):
        pl.semaphore_signal(
            barrier, inc=1, device_id=coordinates(target(step), axes), device_id_type=MESH
        )
        return carry

    lax.fori_loop(1, count, greet, 0)
    pl.semaphore_wait(barrier, count)

    def beside(step):
        slot = target(step)
        return pltpu.make_async_remote_copy(
            src_ref=x_ref.at[slot // inner, 1 - core, lax.rem(slot, inner)],
            dst_ref=got.at[slot],
            send_sem=core_s.at[slot],
            recv_sem=core_r.at[slot],
            device_id=partner,
            device_id_type=MESH,
        )

    def far(step):
        slot = target(step)
        return pltpu.make_async_remote_copy(
            src_ref=mine.at[slot],
            dst_ref=o_ref.at[me],
            send_sem=far_s.at[step],
            recv_sem=far_r.at[step],
            device_id=coordinates(slot, axes),
            device_id_type=MESH,
        )

    def far_in(step):
        source = lax.rem(me - step + count, count)
        return pltpu.make_async_remote_copy(
            src_ref=mine.at[source],
            dst_ref=o_ref.at[source],
            send_sem=far_s.at[step],
            recv_sem=far_r.at[step],
            device_id=coordinates(source, axes),
            device_id_type=MESH,
        )

    def total(slot):
        own = x_ref[slot // inner, core, lax.rem(slot, inner)]
        beside_sum = own.astype(jnp.float32) + got[slot].astype(jnp.float32)
        return beside_sum.astype(jnp.bfloat16)

    def begin(step, carry):
        beside(step).start()
        return carry

    def send(step, carry):
        beside(step).wait_recv()
        mine[target(step)] = total(target(step))
        far(step).start()
        return carry

    def finish(step, carry):
        far_in(step).wait_recv()
        far(step).wait_send()
        beside(step).wait_send()
        return carry

    lax.fori_loop(1, count + 1, begin, 0)
    lax.fori_loop(1, count, send, 0)
    beside(0).wait_recv()
    o_ref[me] = total(me)
    lax.fori_loop(1, count, finish, 0)
    beside(0).wait_send()


def reduce_cores(value, axes, collective_id):
    count = value.shape[0] * value.shape[2]
    shape = (count,) + value.shape[3:]
    sems = pltpu.SemaphoreType.DMA((count,))
    return pl.pallas_call(
        functools.partial(reduce_kernel, axes),
        out_shape=jax.ShapeDtypeStruct(shape, value.dtype),
        in_specs=[pl.BlockSpec(memory_space=pltpu.VMEM)],
        out_specs=pl.BlockSpec(memory_space=pltpu.VMEM),
        scratch_shapes=[
            pltpu.VMEM(shape, value.dtype),
            pltpu.VMEM(shape, value.dtype),
            sems,
            sems,
            sems,
            sems,
        ],
        compiler_params=pltpu.CompilerParams(collective_id=collective_id, has_side_effects=True),
        cost_estimate=pl.CostEstimate(
            flops=0, bytes_accessed=8 * math.prod(shape) + 4000000, transcendentals=0
        ),
    )(value)


def flat_position(axes):
    position = 0
    for axis in axes:
        position = position * lax.axis_size(axis) + lax.axis_index(axis)
    return position


def coordinates(position, axes):
    found = {}
    for axis in reversed(axes):
        size = lax.axis_size(axis)
        found[axis] = lax.rem(position, size)
        position = position // size
    return found


def count_of(axes):
    return math.prod(lax.axis_size(axis) for axis in axes)


def ring_kernel(axis, spread, x_ref, o_ref, hop_s, hop_r, x_s, x_r, c_s, c_r, f_s, f_r, local_sem):
    size = lax.axis_size(axis)
    me = lax.axis_index(axis)
    last = size // 2
    halved = size % 2 == 0
    sides = lax.axis_size("ulysses") if spread else 1
    row = lax.axis_index("ulysses")
    core = lax.axis_index("cfg")
    partner = {"ulysses": row, "cfg": 1 - core}
    base = o_ref.at[row * 2 + core] if spread else o_ref

    def at(offset):
        return lax.rem(me + offset + size, size)

    def aside(step):
        return {"ulysses": lax.rem(row + step, sides), "cfg": core}

    barrier = pltpu.get_barrier_semaphore()
    for way in (1, -1):
        pl.semaphore_signal(barrier, inc=1, device_id={axis: at(way)}, device_id_type=MESH)
    if spread:
        for step in range(1, sides):
            pl.semaphore_signal(barrier, inc=1, device_id=aside(step), device_id_type=MESH)
        pl.semaphore_signal(barrier, inc=1, device_id=partner, device_id_type=MESH)
    own = pltpu.make_async_copy(x_ref, base.at[me], local_sem)
    own.start()
    pl.semaphore_wait(barrier, 2 + (sides if spread else 0))

    def part(ref, way, step):
        if halved and step == last:
            return ref.at[0 if way == 1 else 1]
        return ref

    def hop(way, step):
        slot = at(-way * (step - 1))
        source = x_ref if step == 1 else base.at[slot]
        return pltpu.make_async_remote_copy(
            src_ref=part(source, way, step),
            dst_ref=part(base.at[slot], way, step),
            send_sem=hop_s.at[(way + 1) // 2, step],
            recv_sem=hop_r.at[(way + 1) // 2, step],
            device_id={axis: at(way)},
            device_id_type=MESH,
        )

    def hop_in(way, step):
        slot = base.at[at(-way * step)]
        return pltpu.make_async_remote_copy(
            src_ref=part(slot, way, step),
            dst_ref=part(slot, way, step),
            send_sem=hop_s.at[(way + 1) // 2, step],
            recv_sem=hop_r.at[(way + 1) // 2, step],
            device_id={axis: at(-way)},
            device_id_type=MESH,
        )

    def send(order, offset, step):
        slot = at(offset)
        return pltpu.make_async_remote_copy(
            src_ref=x_ref if order == 0 else base.at[slot],
            dst_ref=base.at[slot],
            send_sem=x_s.at[order, step] if step else c_s.at[order],
            recv_sem=x_r.at[order, step] if step else c_r.at[order],
            device_id=aside(step) if step else partner,
            device_id_type=MESH,
        )

    def across_in(order, offset, step):
        source = lax.rem(row - step + sides, sides)
        block = o_ref.at[source * 2 + core, at(offset)]
        return pltpu.make_async_remote_copy(
            src_ref=block,
            dst_ref=block,
            send_sem=x_s.at[order, step],
            recv_sem=x_r.at[order, step],
            device_id=aside(step),
            device_id_type=MESH,
        )

    def forward(order, offset, step, side):
        source = lax.rem(row - step + sides, sides)
        block = o_ref.at[source * 2 + side, at(offset)]
        return pltpu.make_async_remote_copy(
            src_ref=block,
            dst_ref=block,
            send_sem=f_s.at[order, step],
            recv_sem=f_r.at[order, step],
            device_id=partner,
            device_id_type=MESH,
        )

    def beside_in(order, offset):
        block = o_ref.at[row * 2 + 1 - core, at(offset)]
        return pltpu.make_async_remote_copy(
            src_ref=block,
            dst_ref=block,
            send_sem=c_s.at[order],
            recv_sem=c_r.at[order],
            device_id=partner,
            device_id_type=MESH,
        )

    steps = last
    offsets = [0]
    for way in (1, -1):
        hop(way, 1).start()
    sent = []

    def pass_on(order, offset):
        if spread:
            for step in list(range(1, sides)) + [0]:
                send(order, offset, step).start()
            sent.append((order, offset))

    def relay(order, offset):
        for step in range(1, sides):
            across_in(order, offset, step).wait_recv()
            forward(order, offset, step, core).start()

    pass_on(0, 0)
    relayed = 0
    for step in range(1, steps + 1):
        final = halved and step == last
        for way in (1, -1):
            hop_in(way, step).wait_recv()
            if step < steps:
                hop(way, step + 1).start()
            if not final:
                offsets.append(-way * step)
                pass_on(len(offsets) - 1, offsets[-1])
        if final:
            offsets.append(step)
            pass_on(len(offsets) - 1, step)
        if spread:
            while relayed < len(offsets) - 2:
                relay(relayed, offsets[relayed])
                relayed += 1
    if spread:
        while relayed < len(offsets):
            relay(relayed, offsets[relayed])
            relayed += 1
    for step in range(1, steps + 1):
        for way in (1, -1):
            hop(way, step).wait_send()
    for order, offset in sent:
        for step in range(sides):
            send(order, offset, step).wait_send()
        for step in range(1, sides):
            forward(order, offset, step, core).wait_send()
            forward(order, offset, step, 1 - core).wait_recv()
        beside_in(order, offset).wait_recv()
    own.wait()


def ring_gather(value, axis, spread, collective_id):
    size = lax.axis_size(axis)
    sides = lax.axis_size("ulysses")
    shape = (size,) + value.shape
    if spread:
        shape = (sides * 2,) + shape
    space = pl.ANY if spread else pltpu.VMEM
    hops = pltpu.SemaphoreType.DMA((2, size // 2 + 1))
    across = pltpu.SemaphoreType.DMA((size, sides))
    beside = pltpu.SemaphoreType.DMA((size,))
    return pl.pallas_call(
        functools.partial(ring_kernel, axis, spread),
        out_shape=jax.ShapeDtypeStruct(shape, value.dtype),
        in_specs=[pl.BlockSpec(memory_space=space)],
        out_specs=pl.BlockSpec(memory_space=space),
        scratch_shapes=[hops, hops, across, across, beside, beside, across, across]
        + [pltpu.SemaphoreType.DMA],
        compiler_params=pltpu.CompilerParams(collective_id=collective_id, has_side_effects=True),
        cost_estimate=pl.CostEstimate(
            flops=0, bytes_accessed=8 * math.prod(shape) + 4000000, transcendentals=0
        ),
    )(value)


def silu(value):
    return value / (1.0 + jnp.exp(-value))


def front_kernel(
    time_cols,
    sin_ref,
    pooled_ref,
    len_ref,
    tw_hbm,
    ts_hbm,
    mw_hbm,
    x_ref,
    t_all,
    mod_ref,
    o_ref,
    m_all,
    tw_ref,
    ts_ref,
    mw_ref,
    load_s,
    t_s,
    t_r,
    m_s,
    m_r,
    hop_s,
    hop_r,
    x_s,
    x_r,
    c_s,
    c_r,
    f_s,
    f_r,
    local_sem,
):
    axis = "blk"
    axes = ("blk", "ulysses", "cfg")
    count = count_of(axes)
    place = flat_position(axes)
    size = lax.axis_size(axis)
    me = lax.axis_index(axis)
    last = size // 2
    halved = size % 2 == 0
    sides = lax.axis_size("ulysses")
    row = lax.axis_index("ulysses")
    core = lax.axis_index("cfg")
    partner = {"ulysses": row, "cfg": 1 - core}
    base = o_ref.at[row * 2 + core]

    loads = [
        pltpu.make_async_copy(tw_hbm, tw_ref, load_s.at[0]),
        pltpu.make_async_copy(ts_hbm, ts_ref, load_s.at[1]),
        pltpu.make_async_copy(mw_hbm, mw_ref, load_s.at[2]),
    ]
    for load in loads:
        load.start()
    own = pltpu.make_async_copy(x_ref, base.at[me], local_sem)
    own.start()

    def at(offset):
        return lax.rem(me + offset + size, size)

    def aside(step):
        return {"ulysses": lax.rem(row + step, sides), "cfg": core}

    barrier = pltpu.get_barrier_semaphore()

    def greet(step, carry):
        pl.semaphore_signal(
            barrier,
            inc=1,
            device_id=coordinates(lax.rem(place + step, count), axes),
            device_id_type=MESH,
        )
        return carry

    lax.fori_loop(1, count, greet, 0)

    def outgoing(ref, send, recv, step):
        return pltpu.make_async_remote_copy(
            src_ref=ref.at[place],
            dst_ref=ref.at[place],
            send_sem=send.at[step],
            recv_sem=recv.at[step],
            device_id=coordinates(lax.rem(place + step, count), axes),
            device_id_type=MESH,
        )

    def incoming(ref, send, recv, step):
        source = lax.rem(place - step + count, count)
        return pltpu.make_async_remote_copy(
            src_ref=ref.at[source],
            dst_ref=ref.at[source],
            send_sem=send.at[step],
            recv_sem=recv.at[step],
            device_id=coordinates(source, axes),
            device_id_type=MESH,
        )

    def send_all(ref, send, recv):
        def begin(step, carry):
            outgoing(ref, send, recv, step).start()
            return carry

        lax.fori_loop(1, count, begin, 0)

    def wait_all(ref, send, recv):
        def finish(step, carry):
            incoming(ref, send, recv, step).wait_recv()
            outgoing(ref, send, recv, step).wait_send()
            return carry

        lax.fori_loop(1, count, finish, 0)

    def part(ref, way, step):
        if halved and step == last:
            return ref.at[0 if way == 1 else 1]
        return ref

    def hop(way, step):
        slot = at(-way * (step - 1))
        source = x_ref if step == 1 else base.at[slot]
        return pltpu.make_async_remote_copy(
            src_ref=part(source, way, step),
            dst_ref=part(base.at[slot], way, step),
            send_sem=hop_s.at[(way + 1) // 2, step],
            recv_sem=hop_r.at[(way + 1) // 2, step],
            device_id={axis: at(way)},
            device_id_type=MESH,
        )

    def hop_in(way, step):
        slot = base.at[at(-way * step)]
        return pltpu.make_async_remote_copy(
            src_ref=part(slot, way, step),
            dst_ref=part(slot, way, step),
            send_sem=hop_s.at[(way + 1) // 2, step],
            recv_sem=hop_r.at[(way + 1) // 2, step],
            device_id={axis: at(-way)},
            device_id_type=MESH,
        )

    def send(order, offset, step):
        slot = at(offset)
        return pltpu.make_async_remote_copy(
            src_ref=x_ref if order == 0 else base.at[slot],
            dst_ref=base.at[slot],
            send_sem=x_s.at[order, step] if step else c_s.at[order],
            recv_sem=x_r.at[order, step] if step else c_r.at[order],
            device_id=aside(step) if step else partner,
            device_id_type=MESH,
        )

    def across_in(order, offset, step):
        source = lax.rem(row - step + sides, sides)
        block = o_ref.at[source * 2 + core, at(offset)]
        return pltpu.make_async_remote_copy(
            src_ref=block,
            dst_ref=block,
            send_sem=x_s.at[order, step],
            recv_sem=x_r.at[order, step],
            device_id=aside(step),
            device_id_type=MESH,
        )

    def forward(order, offset, step, side):
        source = lax.rem(row - step + sides, sides)
        block = o_ref.at[source * 2 + side, at(offset)]
        return pltpu.make_async_remote_copy(
            src_ref=block,
            dst_ref=block,
            send_sem=f_s.at[order, step],
            recv_sem=f_r.at[order, step],
            device_id=partner,
            device_id_type=MESH,
        )

    def beside_in(order, offset):
        block = o_ref.at[row * 2 + 1 - core, at(offset)]
        return pltpu.make_async_remote_copy(
            src_ref=block,
            dst_ref=block,
            send_sem=c_s.at[order],
            recv_sem=c_r.at[order],
            device_id=partner,
            device_id_type=MESH,
        )

    loads[0].wait()
    hidden = jnp.dot(sin_ref[...], tw_ref[...], preferred_element_type=jnp.float32)
    hidden = silu(hidden).astype(jnp.bfloat16)
    loads[1].wait()
    mine = jnp.dot(hidden, ts_ref[...], preferred_element_type=jnp.float32)[0:1]
    length = jnp.broadcast_to(len_ref[...], (1, t_all.shape[2] - time_cols))
    t_all[place] = jnp.concatenate([mine, length], axis=1)
    pl.semaphore_wait(barrier, count - 1)
    send_all(t_all, t_s, t_r)

    steps = last
    offsets = [0]
    for way in (1, -1):
        hop(way, 1).start()
    sent = []

    def pass_on(order, offset):
        for step in list(range(1, sides)) + [0]:
            send(order, offset, step).start()
        sent.append((order, offset))

    def relay(order, offset):
        for step in range(1, sides):
            across_in(order, offset, step).wait_recv()
            forward(order, offset, step, core).start()

    pass_on(0, 0)

    wait_all(t_all, t_s, t_r)
    embed = jnp.concatenate([t_all[i][:, :time_cols] for i in range(count)], axis=1)
    acted = silu(embed + pooled_ref[...]).astype(jnp.bfloat16)
    loads[2].wait()
    mods = jnp.dot(acted, mw_ref[...], preferred_element_type=jnp.float32)
    m_all[place] = mods[0 : m_all.shape[1]]
    send_all(m_all, m_s, m_r)

    relayed = 0
    for step in range(1, steps + 1):
        final = halved and step == last
        for way in (1, -1):
            hop_in(way, step).wait_recv()
            if step < steps:
                hop(way, step + 1).start()
            if not final:
                offsets.append(-way * step)
                pass_on(len(offsets) - 1, offsets[-1])
        if final:
            offsets.append(step)
            pass_on(len(offsets) - 1, step)
        while relayed < len(offsets) - 2:
            relay(relayed, offsets[relayed])
            relayed += 1
    wait_all(m_all, m_s, m_r)
    mod_ref[...] = jnp.concatenate([m_all[i] for i in range(count)], axis=1)
    while relayed < len(offsets):
        relay(relayed, offsets[relayed])
        relayed += 1
    for step in range(1, steps + 1):
        for way in (1, -1):
            hop(way, step).wait_send()
    for order, offset in sent:
        for step in range(sides):
            send(order, offset, step).wait_send()
        for step in range(1, sides):
            forward(order, offset, step, core).wait_send()
            forward(order, offset, step, 1 - core).wait_recv()
        beside_in(order, offset).wait_recv()
    own.wait()


def front(sinusoid_rows, pooled, length, time_weight, time_second, mod_weight, tokens):
    axes = ("blk", "ulysses", "cfg")
    count = count_of(axes)
    size = lax.axis_size("blk")
    sides = lax.axis_size("ulysses")
    branches, _ = pooled.shape
    time_cols = time_second.shape[1]
    mod_cols = mod_weight.shape[1]
    padded = -(-(time_cols + 1) // 128) * 128
    hops = pltpu.SemaphoreType.DMA((2, size // 2 + 1))
    across = pltpu.SemaphoreType.DMA((size, sides))
    beside = pltpu.SemaphoreType.DMA((size,))
    peers = pltpu.SemaphoreType.DMA((count,))
    vmem = pl.BlockSpec(memory_space=pltpu.VMEM)
    anywhere = pl.BlockSpec(memory_space=pl.ANY)
    sin_rows = jnp.broadcast_to(sinusoid_rows, (16, sinusoid_rows.shape[1]))
    pooled_rows = jnp.pad(pooled, ((0, 16 - branches), (0, 0)))
    return pl.pallas_call(
        functools.partial(front_kernel, time_cols),
        out_shape=(
            jax.ShapeDtypeStruct((count, 1, padded), jnp.float32),
            jax.ShapeDtypeStruct((branches, count * mod_cols), jnp.float32),
            jax.ShapeDtypeStruct((sides * 2, size) + tokens.shape, tokens.dtype),
        ),
        in_specs=[vmem] * 3 + [anywhere] * 4,
        out_specs=(vmem, vmem, anywhere),
        scratch_shapes=[
            pltpu.VMEM((count, branches, mod_cols), jnp.float32),
            pltpu.VMEM(time_weight.shape, time_weight.dtype),
            pltpu.VMEM(time_second.shape, time_second.dtype),
            pltpu.VMEM(mod_weight.shape, mod_weight.dtype),
            pltpu.SemaphoreType.DMA((3,)),
            peers,
            peers,
            peers,
            peers,
            hops,
            hops,
            across,
            across,
            beside,
            beside,
            across,
            across,
            pltpu.SemaphoreType.DMA,
        ],
        compiler_params=pltpu.CompilerParams(
            collective_id=0, has_side_effects=True, vmem_limit_bytes=20 * 2**20
        ),
        cost_estimate=pl.CostEstimate(
            flops=0, bytes_accessed=8 * count * math.prod(tokens.shape), transcendentals=0
        ),
        name="front",
    )(sin_rows, pooled_rows, length, time_weight, time_second, mod_weight, tokens)


def normed(values, shift, scale):
    average = jnp.mean(values, axis=-1, keepdims=True)
    centred = values - average
    variance = jnp.mean(centred * centred, axis=-1, keepdims=True)
    return (centred * lax.rsqrt(variance + LN_EPS) * (1.0 + scale) + shift).astype(jnp.bfloat16)


def unit_heads(values, gains, same_head, head_size):
    parts = []
    lanes = same_head.shape[0]
    for first in range(0, values.shape[1], lanes):
        piece = values[:, first : first + lanes]
        square = piece * piece
        high = square.astype(jnp.bfloat16)
        low = (square - high.astype(jnp.float32)).astype(jnp.bfloat16)
        total = jnp.dot(high, same_head, preferred_element_type=jnp.float32)
        total = total + jnp.dot(low, same_head, preferred_element_type=jnp.float32)
        scale = lax.rsqrt(total * (1.0 / head_size) + RMS_EPS)
        parts.append((piece * scale * gains[:, first : first + lanes]).astype(jnp.bfloat16))
    return jnp.concatenate(parts, axis=1)


def block_kernel(
    head_size,
    rows,
    slots,
    tok_ref,
    mod_ref,
    live_ref,
    pw_ref,
    ow_ref,
    gain_ref,
    o_ref,
    h_ref,
    ht_ref,
    q_ref,
    k_ref,
    v_ref,
    mix_ref,
):
    quads, _, halves, _, width = tok_ref.shape
    sides = quads // 2
    blocks = pl.num_programs(0)
    block = pl.program_id(0)
    me = lax.axis_index("blk")
    inner = pw_ref.shape[2]
    img = sides * halves * rows
    lanes = 2 * head_size
    chunk = img
    while chunk % 32 == 0 and 8 * chunk * k_ref.shape[1] > 2**21:
        chunk //= 2
    head_row = lax.broadcasted_iota(jnp.int32, (lanes, lanes), 0) // head_size
    head_col = lax.broadcasted_iota(jnp.int32, (lanes, lanes), 1) // head_size
    same_head = jnp.where(head_row == head_col, 1.0, 0.0).astype(jnp.bfloat16)

    def mod(branch, index):
        return mod_ref[branch : branch + 1, index * width : (index + 1) * width]

    for branch in range(2):
        for side in range(sides):
            for half in range(halves):
                x = tok_ref[side * 2 + branch, 0, half].astype(jnp.float32)
                first = (branch * sides + side) * halves + half
                h_ref[first * rows : (first + 1) * rows] = normed(
                    x[:rows], mod(branch, 0), mod(branch, 1)
                )
                spot = ((branch * blocks + block) * sides + side) * halves + half
                ht_ref[spot] = normed(x[rows:], mod(branch, 4), mod(branch, 3))

    keys = jnp.dot(h_ref[...], pw_ref[1], preferred_element_type=jnp.float32)
    keys = unit_heads(keys, gain_ref[1:2], same_head, head_size)
    values = jnp.dot(h_ref[...], pw_ref[2], preferred_element_type=jnp.float32)
    values = values.astype(jnp.bfloat16)
    start = pl.multiple_of(block * img, img)
    for branch in range(2):
        k_ref[branch, pl.ds(start, img)] = keys[branch * img : (branch + 1) * img]
        v_ref[branch, pl.ds(start, img)] = values[branch * img : (branch + 1) * img]

    @pl.when(block == me)
    def _():
        found = jnp.dot(h_ref[...], pw_ref[0], preferred_element_type=jnp.float32)
        found = unit_heads(found, gain_ref[0:1], same_head, head_size)
        q_ref[...] = found * jnp.asarray(1.0 / math.sqrt(head_size), jnp.bfloat16)

    @pl.when(block == blocks - 1)
    def _():
        text = ht_ref[...].reshape(-1, width)
        keys = jnp.dot(text, pw_ref[3], preferred_element_type=jnp.float32)
        keys = unit_heads(keys, gain_ref[2:3], same_head, head_size)
        values = jnp.dot(text, pw_ref[4], preferred_element_type=jnp.float32)
        values = values.astype(jnp.bfloat16)
        ahead = k_ref.shape[1] - slots
        for branch in range(2):
            k_ref[branch, ahead:] = keys[branch * slots : (branch + 1) * slots]
            v_ref[branch, ahead:] = values[branch * slots : (branch + 1) * slots]
        low = lax.broadcasted_iota(jnp.int32, (1, lanes), 1) < head_size
        for branch in range(2):
            live = live_ref[branch : branch + 1] > 0.0
            for first in range(0, inner, lanes):
                here = slice(first, first + lanes)

                def attend(step, carry, branch=branch, here=here, live=live):
                    begin = branch * img + step * chunk
                    if chunk < img:
                        begin = pl.multiple_of(begin, chunk)
                    queries = q_ref[pl.ds(begin, chunk), here]
                    nothing = jnp.zeros_like(queries)
                    pair = jnp.concatenate(
                        [jnp.where(low, queries, nothing), jnp.where(low, nothing, queries)], axis=0
                    )
                    scores = lax.dot_general(
                        pair,
                        k_ref[branch, :, here],
                        (((1,), (1,)), ((), ())),
                        preferred_element_type=jnp.float32,
                    )
                    scores = jnp.where(live, scores, NEG_FILL)
                    largest = jnp.max(scores, axis=1, keepdims=True)
                    weights = jnp.exp(scores - largest)
                    denominator = jnp.sum(weights, axis=1, keepdims=True)
                    update = jnp.dot(
                        weights.astype(jnp.bfloat16),
                        v_ref[branch, :, here],
                        preferred_element_type=jnp.float32,
                    )
                    update = update / denominator
                    both = jnp.where(low, update[:chunk], update[chunk:]).astype(jnp.bfloat16)
                    mix_ref[pl.ds(begin, chunk), here] = both
                    return carry

                if chunk == img:
                    attend(0, 0)
                else:
                    lax.fori_loop(0, img // chunk, attend, 0)
        out = jnp.dot(mix_ref[...], ow_ref[...], preferred_element_type=jnp.float32)
        out = out.astype(jnp.bfloat16)
        tokens = halves * rows
        for branch in range(2):
            for side in range(sides):
                first = (branch * sides + side) * tokens
                o_ref[side, branch, 0] = out[first : first + tokens]


def block_attention(tokens, mods, live, proj_weight, out_weight, gains, head_size, rows):
    quads, blocks, halves, span, width = tokens.shape
    sides = quads // 2
    inner = proj_weight.shape[2]
    img = sides * halves * rows
    slots = blocks * sides * halves * (span - rows)
    keys = blocks * img + slots
    resident = pl.BlockSpec(memory_space=pltpu.VMEM)
    out_shape = (sides, 2, 1, halves * rows, width)
    return pl.pallas_call(
        functools.partial(block_kernel, head_size, rows, slots),
        grid=(blocks,),
        out_shape=jax.ShapeDtypeStruct(out_shape, jnp.bfloat16),
        in_specs=[
            pl.BlockSpec((quads, 1, halves, span, width), lambda z: (0, z, 0, 0, 0)),
            resident,
            resident,
            resident,
            resident,
            resident,
        ],
        out_specs=resident,
        scratch_shapes=[
            pltpu.VMEM((2 * img, width), jnp.bfloat16),
            pltpu.VMEM((2 * blocks * sides * halves, span - rows, width), jnp.bfloat16),
            pltpu.VMEM((2 * img, inner), jnp.bfloat16),
            pltpu.VMEM((2, keys, inner), jnp.bfloat16),
            pltpu.VMEM((2, keys, inner), jnp.bfloat16),
            pltpu.VMEM((2 * img, inner), jnp.bfloat16),
        ],
        compiler_params=pltpu.CompilerParams(
            dimension_semantics=("arbitrary",), vmem_limit_bytes=60 * 2**20
        ),
        cost_estimate=pl.CostEstimate(
            flops=8 * 2 * blocks * img * width * inner,
            bytes_accessed=2 * math.prod(tokens.shape),
            transcendentals=0,
        ),
        name="block_attention",
    )(tokens, mods, live, proj_weight, out_weight, gains)


class WeightRing:
    def __init__(self, piece, axis, across):
        self.axis, self.across = axis, across
        self.size = lax.axis_size(axis)
        self.parts = lax.axis_size(across)
        self.me = lax.axis_index(axis)
        self.part = lax.axis_index(across)
        self.rows = piece.shape[0]
        self.share = self.rows // self.parts
        self.up = [(source, (source + 1) % self.size) for source in range(self.size)]
        self.down = [(source, (source - 1) % self.size) for source in range(self.size)]
        whole = jnp.zeros((self.size * self.rows,) + piece.shape[1:], piece.dtype)
        self.whole = lax.dynamic_update_slice_in_dim(whole, piece, self.me * self.rows, 0)
        own = lax.dynamic_slice_in_dim(piece, self.part * self.share, self.share, 0)
        self.upward = self.downward = own

    def place(self, block, owner, offset):
        for step in range(self.parts):
            if step:
                pairs = [(part, (part + step) % self.parts) for part in range(self.parts)]
                moved = lax.ppermute(block, self.across, pairs)
            else:
                moved = block
            origin = lax.rem(self.part - step + self.parts, self.parts)
            start = owner * self.rows + origin * self.share + offset
            self.whole = lax.dynamic_update_slice_in_dim(self.whole, moved, start, 0)

    def hop(self, step, after):
        size, me = self.size, self.me
        self.upward, self.downward, after = lax.optimization_barrier(
            (self.upward, self.downward, after)
        )
        if step <= (size - 1) // 2:
            self.upward = lax.ppermute(self.upward, self.axis, self.up)
            self.downward = lax.ppermute(self.downward, self.axis, self.down)
            self.place(self.upward, lax.rem(me - step + size, size), 0)
            self.place(self.downward, lax.rem(me + step, size), 0)
        else:
            half = self.share // 2
            far = lax.rem(me + step, size)
            low = lax.ppermute(self.upward[:half], self.axis, self.up)
            high = lax.ppermute(self.downward[half:], self.axis, self.down)
            self.place(jnp.concatenate([low, high], axis=0), far, 0)
        return after


def body(
    img_tokens,
    text_tokens,
    text_lengths,
    timestep,
    pooled,
    time_weight,
    time_second,
    mod_weight,
    proj_weight,
    out_weight,
    expand_weight,
    reduce_weight,
    qk_gain,
    final_weight,
):
    model_width = img_tokens.shape[3]
    prompts = img_tokens.shape[1]
    branches = pooled.shape[0]
    branch = lax.axis_index("cfg")
    blocks = lax.axis_size("blk")
    sides = lax.axis_size("ulysses")
    ring = WeightRing(expand_weight, "blk", "groups")
    inner_local = proj_weight.shape[2]
    head_size = qk_gain.shape[1]
    image_rows = img_tokens[0]
    text_rows = text_tokens[0]
    token_count = image_rows.shape[1]
    slot_count = text_rows.shape[1]
    half_rows = token_count // 2
    half_text = -(-slot_count // 2)
    text_pad = -(-half_text // 8) * 8
    text_halves = jnp.pad(text_rows[0], ((0, 2 * half_text - slot_count), (0, 0)))
    text_halves = jnp.pad(
        text_halves.reshape(2, half_text, model_width), ((0, 0), (0, text_pad - half_text), (0, 0))
    )
    packed = jnp.concatenate(
        [image_rows.reshape(2, half_rows, model_width), text_halves], axis=1
    )
    sinusoid_rows = sinusoid(timestep, time_weight.shape[0]).astype(jnp.bfloat16)
    times, mods, tokens = front(
        sinusoid_rows,
        pooled.reshape(branches, model_width),
        text_lengths.astype(jnp.float32),
        time_weight,
        time_second,
        mod_weight,
        packed,
    )
    time_width = time_second.shape[1]
    lengths = times[:branches, 0, time_width].astype(jnp.int32)
    mods = ring.hop(1, mods)
    spot = jnp.arange(blocks * sides * 2 * text_pad, dtype=jnp.int32)
    within = lax.rem(spot, text_pad)
    half = lax.rem(spot // text_pad, 2)
    owner = spot // (2 * text_pad)
    slot = owner * slot_count + half * half_text + within
    real = (within < half_text) & (half * half_text + within < slot_count)
    usable = (slot[None, :] < lengths[:, None]) & real[None, :]
    live = jnp.concatenate(
        [jnp.ones((branches, blocks * sides * token_count), jnp.float32), usable.astype(jnp.float32)],
        axis=1,
    )
    gains = jnp.tile(qk_gain, (1, inner_local // head_size))
    out_terms = block_attention(
        tokens, mods, live, proj_weight, out_weight, gains, head_size, half_rows
    )
    own_mod = lax.dynamic_index_in_dim(mods, branch, 0, keepdims=False)
    own_mod = own_mod.reshape(prompts, 10, model_width)
    for step in range(2, blocks // 2 + 1):
        out_terms = ring.hop(step, out_terms)
    out_terms = reduce_cores(out_terms, ("ulysses",), 3)
    attended = jnp.sum(out_terms.astype(jnp.float32), axis=0)
    attended = attended.reshape(prompts, token_count, model_width)
    residual = image_rows.astype(jnp.float32) + own_mod[:, 2:3] * attended
    feed_input = modulate(residual, own_mod[:, 7:8], own_mod[:, 8:9]).reshape(
        prompts * token_count, model_width
    )
    feed_halves = feed_input.reshape(2, -1, model_width)
    feed_all = ring_gather(feed_halves, "blk", True, 4)
    feed_all = feed_all.reshape(-1, model_width)
    pre_active = jnp.dot(feed_all, ring.whole, preferred_element_type=jnp.float32)
    feed_hidden = jax.nn.gelu(pre_active, approximate=True).astype(jnp.bfloat16)
    feed_hidden = lax.optimization_barrier(feed_hidden)
    feed_terms = jnp.dot(feed_hidden, reduce_weight, preferred_element_type=jnp.float32)
    feed_terms = feed_terms.astype(jnp.bfloat16).reshape(
        sides, branches, blocks, prompts * token_count, -1
    )
    feed_terms = reduce_cores(feed_terms, ("ulysses", "blk"), 5)
    feed_terms = feed_terms.reshape(sides, blocks, prompts * token_count, -1)
    feed_out = jnp.sum(feed_terms.astype(jnp.float32), axis=0).transpose(1, 0, 2)
    second_residual = residual + own_mod[:, 9:10] * feed_out.reshape(
        prompts, token_count, model_width
    )
    final_rows = modulate(second_residual, own_mod[:, 6:7], own_mod[:, 5:6])
    noise = jnp.einsum("prd,dc->prc", final_rows, final_weight, preferred_element_type=jnp.float32)
    latent_channels = final_weight.shape[1] // 4
    noise_own = noise.reshape(prompts, token_count, 2, 2, latent_channels).transpose(0, 4, 2, 1, 3)
    noise_own = noise_own.reshape(prompts, latent_channels, 2, 2 * token_count)
    kept_row = lax.dynamic_slice_in_dim(noise_own, branch, 1, 2)
    sent_row = lax.dynamic_slice_in_dim(noise_own, 1 - branch, 1, 2)
    noise_pair = from_partner(sent_row, "cfg", 0)
    noise_cond = jnp.where(branch == 0, kept_row, noise_pair)
    noise_uncond = jnp.where(branch == 0, noise_pair, kept_row)
    return noise_uncond + GUIDANCE * (noise_cond - noise_uncond)


def solution(mesh):
    in_specs = (
        P("cfg", "groups", ("blk", "ulysses"), None),
        P("cfg", "groups", ("blk", "ulysses"), None),
        P("cfg", "groups"),
        P("groups"),
        P(None, "groups", None),
        P(),
        P(None, ("blk", "ulysses", "cfg")),
        P(None, ("blk", "ulysses", "cfg")),
        P(None, None, ("ulysses", "cfg")),
        P(("ulysses", "cfg"), None),
        P("blk", ("ulysses", "cfg")),
        P(("ulysses", "cfg"), "blk"),
        P(),
        P(),
    )
    out_specs = P("groups", None, ("blk", "ulysses", "cfg"), None)


    return jax.shard_map(body, mesh=mesh, in_specs=in_specs, out_specs=out_specs, check_vma=False)
```

```python
import functools
import math

import jax
import jax.numpy as jnp
from jax import lax
from jax.experimental import pallas as pl
from jax.experimental.pallas import tpu as pltpu
from jax.sharding import PartitionSpec as P

GUIDANCE = 3.5
LN_EPS = 1e-06
RMS_EPS = 1e-06
NEG_FILL = -1e30
LANES = 128
MESH = pl.DeviceIdType.MESH


def sinusoid(timestep, feature_count):
    half_width = feature_count // 2
    frequency = jnp.exp(-math.log(10000.0) * jnp.arange(half_width, dtype=jnp.float32) / half_width)
    angles = timestep.astype(jnp.float32)[:, None] * frequency[None, :]
    return jnp.concatenate([jnp.cos(angles), jnp.sin(angles)], axis=1)


def silu(value):
    return value / (1.0 + jnp.exp(-value))


def flat_position(axes):
    position = 0
    for axis in axes:
        position = position * lax.axis_size(axis) + lax.axis_index(axis)
    return position


def coordinates(position, axes):
    found = {}
    for axis in reversed(axes):
        size = lax.axis_size(axis)
        found[axis] = lax.rem(position, size)
        position = position // size
    return found


def count_of(axes):
    return math.prod(lax.axis_size(axis) for axis in axes)


def normed(values, shift, scale):
    average = jnp.mean(values, axis=-1, keepdims=True)
    centred = values - average
    variance = jnp.mean(centred * centred, axis=-1, keepdims=True)
    return (centred * lax.rsqrt(variance + LN_EPS) * (1.0 + scale) + shift).astype(jnp.bfloat16)


def unit_heads(values, gains, same_head, head_size):
    parts = []
    lanes = same_head.shape[0]
    for first in range(0, values.shape[1], lanes):
        piece = values[:, first : first + lanes]
        square = piece * piece
        high = square.astype(jnp.bfloat16)
        low = (square - high.astype(jnp.float32)).astype(jnp.bfloat16)
        total = jnp.dot(high, same_head, preferred_element_type=jnp.float32)
        total = total + jnp.dot(low, same_head, preferred_element_type=jnp.float32)
        scale = lax.rsqrt(total * (1.0 / head_size) + RMS_EPS)
        parts.append((piece * scale * gains[:, first : first + lanes]).astype(jnp.bfloat16))
    return jnp.concatenate(parts, axis=1)


def window(index, share, total, width):
    start = jnp.minimum(index * share // LANES * LANES, total - width)
    return pl.multiple_of(start, LANES)


def window_width(share, total, parts):
    ends = [-(-(index + 1) * share // LANES) - index * share // LANES for index in range(parts)]
    return min(max(ends) * LANES, total)


class Spread:
    def __init__(self, x_ref, o_ref, cut, sems):
        self.x_ref, self.o_ref, self.cut = x_ref, o_ref, cut
        self.hop_s, self.hop_r, self.x_s, self.x_r = sems[:4]
        self.c_s, self.c_r, self.f_s, self.f_r = sems[4:8]
        self.local = sems[8]
        self.size = lax.axis_size("blk")
        self.me = lax.axis_index("blk")
        self.last = self.size // 2
        self.halved = self.size % 2 == 0
        self.sides = lax.axis_size("ulysses")
        self.row = lax.axis_index("ulysses")
        self.core = lax.axis_index("cfg")
        self.partner = {"ulysses": self.row, "cfg": 1 - self.core}
        self.base = o_ref.at[self.row * 2 + self.core]
        self.offsets = [0]
        self.sent = []
        self.own = pltpu.make_async_copy(x_ref, self.base.at[self.me], self.local)

    def at(self, offset):
        return lax.rem(self.me + offset + self.size, self.size)

    def copy(self, source, target, send, recv, device):
        return pltpu.make_async_remote_copy(
            src_ref=source,
            dst_ref=target,
            send_sem=send,
            recv_sem=recv,
            device_id=device,
            device_id_type=MESH,
        )

    def part(self, ref, way, step):
        if self.halved and step == self.last:
            rows = ref.shape[0]
            return ref.at[pl.ds(0, self.cut)] if way == 1 else ref.at[pl.ds(self.cut, rows - self.cut)]
        return ref

    def hop(self, way, step):
        slot = self.at(-way * (step - 1))
        source = self.x_ref if step == 1 else self.base.at[slot]
        sem = ((way + 1) // 2, step)
        return self.copy(
            self.part(source, way, step),
            self.part(self.base.at[slot], way, step),
            self.hop_s.at[sem],
            self.hop_r.at[sem],
            {"blk": self.at(way)},
        )

    def hop_in(self, way, step):
        slot = self.part(self.base.at[self.at(-way * step)], way, step)
        sem = ((way + 1) // 2, step)
        return self.copy(
            slot, slot, self.hop_s.at[sem], self.hop_r.at[sem], {"blk": self.at(-way)}
        )

    def aside(self, step):
        return {"ulysses": lax.rem(self.row + step, self.sides), "cfg": self.core}

    def send(self, order, step):
        slot = self.at(self.offsets[order])
        return self.copy(
            self.x_ref if order == 0 else self.base.at[slot],
            self.base.at[slot],
            self.x_s.at[order, step] if step else self.c_s.at[order],
            self.x_r.at[order, step] if step else self.c_r.at[order],
            self.aside(step) if step else self.partner,
        )

    def across_in(self, order, step):
        source = lax.rem(self.row - step + self.sides, self.sides)
        block = self.o_ref.at[source * 2 + self.core, self.at(self.offsets[order])]
        return self.copy(
            block, block, self.x_s.at[order, step], self.x_r.at[order, step], self.aside(step)
        )

    def forward(self, order, step, side):
        source = lax.rem(self.row - step + self.sides, self.sides)
        block = self.o_ref.at[source * 2 + side, self.at(self.offsets[order])]
        return self.copy(
            block, block, self.f_s.at[order, step], self.f_r.at[order, step], self.partner
        )

    def beside_in(self, order):
        block = self.o_ref.at[self.row * 2 + 1 - self.core, self.at(self.offsets[order])]
        return self.copy(block, block, self.c_s.at[order], self.c_r.at[order], self.partner)

    def pass_on(self, order):
        for step in list(range(1, self.sides)) + [0]:
            self.send(order, step).start()

    def begin(self):
        for way in (1, -1):
            self.hop(way, 1).start()
        self.pass_on(0)

    def advance(self, step):
        final = self.halved and step == self.last
        for way in (1, -1):
            self.hop_in(way, step).wait_recv()
            if step < self.last:
                self.hop(way, step + 1).start()
            if not final:
                self.offsets.append(-way * step)
                self.pass_on(len(self.offsets) - 1)
        if final:
            self.offsets.append(step)
            self.pass_on(len(self.offsets) - 1)

    def relay(self, order):
        for step in range(1, self.sides):
            self.across_in(order, step).wait_recv()
            self.forward(order, step, self.core).start()

    def ready(self, order):
        for step in range(1, self.sides):
            self.forward(order, step, 1 - self.core).wait_recv()
        self.beside_in(order).wait_recv()
        if order == 0:
            self.own.wait()

    def end(self):
        for step in range(1, self.last + 1):
            for way in (1, -1):
                self.hop(way, step).wait_send()
        for order in range(len(self.offsets)):
            for step in range(self.sides):
                self.send(order, step).wait_send()
            for step in range(1, self.sides):
                self.forward(order, step, self.core).wait_send()


def spread_sems():
    size = lax.axis_size("blk")
    hops = pltpu.SemaphoreType.DMA((2, size // 2 + 1))
    across = pltpu.SemaphoreType.DMA((size, lax.axis_size("ulysses")))
    beside = pltpu.SemaphoreType.DMA((size,))
    one = pltpu.SemaphoreType.DMA
    return [hops, hops, across, across, beside, beside, across, across, one]


def greet_all():
    axes = ("blk", "ulysses", "cfg")
    count = count_of(axes)
    place = flat_position(axes)
    groups = lax.axis_size("groups")
    barrier = pltpu.get_barrier_semaphore()

    def greet(step, carry):
        pl.semaphore_signal(
            barrier,
            inc=1,
            device_id=coordinates(lax.rem(place + step, count), axes),
            device_id_type=MESH,
        )
        return carry

    lax.fori_loop(1, count, greet, 0)
    for step in range(1, groups):
        other = lax.rem(lax.axis_index("groups") + step, groups)
        pl.semaphore_signal(barrier, inc=1, device_id={"groups": other}, device_id_type=MESH)
    return barrier, count - 1 + groups - 1


class Shuffle:
    def __init__(self, source, target, sems, parts):
        self.source, self.target, self.parts = source, target, parts
        self.z_s, self.z_r, self.y_s, self.y_r, self.local = sems
        self.size = lax.axis_size("blk")
        self.me = lax.axis_index("blk")
        self.part = lax.axis_index("groups")
        self.rows, self.total = source.shape
        self.share = self.total // self.size
        self.width = target.shape[1]
        self.height = self.rows // parts

    def columns(self, index):
        return pl.ds(window(index, self.share, self.total, self.width), self.width)

    def block(self, index, part):
        start = index * self.rows
        if self.parts > 1:
            start = start + part * self.height
        return self.target.at[pl.ds(pl.multiple_of(start, 8), self.height)]

    def piece(self, index):
        if self.parts == 1:
            return self.source.at[:, self.columns(index)]
        start = pl.multiple_of(self.part * self.height, 8)
        return self.source.at[pl.ds(start, self.height), self.columns(index)]

    def own(self):
        start = pl.multiple_of(self.me * self.rows, 8)
        return pltpu.make_async_copy(
            self.source.at[:, self.columns(self.me)],
            self.target.at[pl.ds(start, self.rows)],
            self.local,
        )

    def remote(self, source, target, send, recv, device):
        return pltpu.make_async_remote_copy(
            src_ref=source,
            dst_ref=target,
            send_sem=send,
            recv_sem=recv,
            device_id=device,
            device_id_type=MESH,
        )

    def out(self, step):
        target = lax.rem(self.me + step, self.size)
        return self.remote(
            self.piece(target),
            self.block(self.me, self.part),
            self.z_s.at[step],
            self.z_r.at[step],
            {"blk": target},
        )

    def into(self, step):
        source = lax.rem(self.me - step + self.size, self.size)
        return self.remote(
            self.block(source, self.part),
            self.block(source, self.part),
            self.z_s.at[step],
            self.z_r.at[step],
            {"blk": source},
        )

    def cross(self, step, turn, arriving):
        origin = lax.rem(self.me - step + self.size, self.size)
        part = self.part
        other = lax.rem(self.part + turn, self.parts)
        if arriving:
            part = other = lax.rem(self.part - turn + self.parts, self.parts)
        block = self.block(origin, part)
        return self.remote(
            block, block, self.y_s.at[step, turn], self.y_r.at[step, turn], {"groups": other}
        )

    def begin(self):
        self.own().start()
        for step in self.order():
            self.out(step).start()

    def order(self):
        steps = []
        for step in range(1, self.size // 2 + 1):
            steps.append(step)
            if self.size - step != step:
                steps.append(self.size - step)
        return steps

    def pass_on(self, steps):
        for step in steps:
            self.into(step).wait_recv()
            for turn in range(1, self.parts):
                self.cross(step, turn, False).start()

    def end(self):
        self.own().wait()
        for step in self.order():
            self.out(step).wait_send()
            for turn in range(1, self.parts):
                self.cross(step, turn, False).wait_send()
                self.cross(step, turn, True).wait_recv()


def shuffle_sems(parts):
    size = lax.axis_size("blk")
    line = pltpu.SemaphoreType.DMA((size,))
    grid = pltpu.SemaphoreType.DMA((size, max(parts, 2)))
    return [line, line, grid, grid, pltpu.SemaphoreType.DMA]


def joint_kernel(cfg, *refs):
    (
        sin_ref, pooled_ref, len_ref, gain_ref, x_ref,
        fw_ref, tw_hbm, ts_hbm, mw_hbm, pw_hbm, ow_hbm, w1_hbm, w2_hbm,
        o_ref, tok_ref, rows_ref, w1_ref, w2_ref, res_ref, feed_ref,
        t_all, m_all, mod_ref, tw_ref, ts_ref, mw_ref, pw_ref, ow_ref,
        stage, h_ref, ht_ref, q_ref, k_ref, v_ref, kt_ref, vt_ref, mix_ref,
        give, got, mine, att, term, gift_in, x_out, x_in, z_out, z_in, noise, noise_in,
        load_s, t_s, t_r, m_s, m_r, core_s, core_r, side_s, side_r, stage_s,
        give_s, give_r, over_s, over_r, line_s, line_r, last_s, last_r, free_c, free_x,
    ) = refs[: cfg["count"]]
    sems = list(refs[cfg["count"] :])
    head_size, slot_count = cfg["head_size"], cfg["slot_count"]
    rows, cut, big = cfg["rows"], cfg["cut"], cfg["big"]
    axes = ("blk", "ulysses", "cfg")
    count = count_of(axes)
    place = flat_position(axes)
    size = lax.axis_size("blk")
    sides = lax.axis_size("ulysses")
    row = lax.axis_index("ulysses")
    core = lax.axis_index("cfg")
    width = x_ref.shape[1]
    inner = pw_ref.shape[2]
    tokens = 2 * rows
    img = sides * tokens
    text = cut - rows
    time_cols = ts_ref.shape[0]
    lanes = 2 * head_size

    loads = [
        pltpu.make_async_copy(source, target, load_s.at[index])
        for index, (source, target) in enumerate(
            [(tw_hbm, tw_ref), (ts_hbm, ts_ref), (mw_hbm, mw_ref), (pw_hbm, pw_ref), (ow_hbm, ow_ref)]
        )
    ]
    for load in loads:
        load.start()
    spread = Spread(x_ref, tok_ref, cut, sems[:9])
    first = Shuffle(w1_hbm, w1_ref, sems[9:14], cfg["parts"])
    second = Shuffle(w2_hbm, w2_ref, sems[14:19], cfg["parts"])
    feed = Spread(feed_ref, rows_ref, rows, sems[19:28])
    if cfg["reuse"]:
        term = mw_ref
    spread.own.start()
    barrier, expected = greet_all()

    def outgoing(ref, send, recv, step):
        return pltpu.make_async_remote_copy(
            src_ref=ref.at[place],
            dst_ref=ref.at[place],
            send_sem=send.at[step],
            recv_sem=recv.at[step],
            device_id=coordinates(lax.rem(place + step, count), axes),
            device_id_type=MESH,
        )

    def incoming(ref, send, recv, step):
        source = lax.rem(place - step + count, count)
        return pltpu.make_async_remote_copy(
            src_ref=ref.at[source],
            dst_ref=ref.at[source],
            send_sem=send.at[step],
            recv_sem=recv.at[step],
            device_id=coordinates(source, axes),
            device_id_type=MESH,
        )

    def send_all(ref, send, recv):
        def begin(step, carry):
            outgoing(ref, send, recv, step).start()
            return carry

        lax.fori_loop(1, count, begin, 0)

    def wait_all(ref, send, recv):
        def finish(step, carry):
            incoming(ref, send, recv, step).wait_recv()
            outgoing(ref, send, recv, step).wait_send()
            return carry

        lax.fori_loop(1, count, finish, 0)

    flip = (((1,), (1,)), ((), ()))
    loads[0].wait()
    hidden = jnp.dot(sin_ref[...], tw_ref[...], preferred_element_type=jnp.float32)
    hidden = silu(hidden).astype(jnp.bfloat16)
    loads[1].wait()
    part = lax.dot_general(hidden, ts_ref[...], flip, preferred_element_type=jnp.float32)[0:1]
    length = jnp.broadcast_to(len_ref[...], (1, t_all.shape[2] - time_cols))
    t_all[place] = jnp.concatenate([part, length], axis=1)
    pl.semaphore_wait(barrier, expected)
    send_all(t_all, t_s, t_r)
    spread.begin()
    wait_all(t_all, t_s, t_r)
    embed = jnp.concatenate([t_all[i][:, :time_cols] for i in range(count)], axis=1)
    acted = silu(embed + pooled_ref[...]).astype(jnp.bfloat16)
    loads[2].wait()
    mods = lax.dot_general(acted, mw_ref[...], flip, preferred_element_type=jnp.float32)
    m_all[place] = mods[0:2]
    send_all(m_all, m_s, m_r)
    spread.advance(1)
    spread.relay(0)
    wait_all(m_all, m_s, m_r)
    for branch in range(2):
        mod_ref[branch] = jnp.concatenate(
            [m_all[i][branch : branch + 1] for i in range(count)], axis=1
        )

    def mod(branch, index):
        return mod_ref[branch, :, index * width : (index + 1) * width]

    head_row = lax.broadcasted_iota(jnp.int32, (lanes, lanes), 0) // head_size
    head_col = lax.broadcasted_iota(jnp.int32, (lanes, lanes), 1) // head_size
    same_head = jnp.where(head_row == head_col, 1.0, 0.0).astype(jnp.bfloat16)

    def project(order):
        slot = spread.at(spread.offsets[order])
        if big:
            fetch = pltpu.make_async_copy(tok_ref.at[:, slot], stage, stage_s)
            fetch.start()
            fetch.wait()

        def tile(side, branch):
            index = side * 2 + branch
            return stage[index] if big else tok_ref[index, slot]

        for branch in range(2):
            for side in range(sides):
                x = tile(side, branch).astype(jnp.float32)
                start = branch * img + side * tokens
                h_ref[start : start + rows] = normed(x[:rows], mod(branch, 0), mod(branch, 1))
                h_ref[start + rows : start + tokens] = normed(
                    x[cut:], mod(branch, 0), mod(branch, 1)
                )
                spot = (branch * size + order) * sides + side
                ht_ref[spot] = normed(x[rows:cut], mod(branch, 4), mod(branch, 3))
        keys = jnp.dot(h_ref[...], pw_ref[1], preferred_element_type=jnp.float32)
        keys = unit_heads(keys, gain_ref[1:2], same_head, head_size)
        values = jnp.dot(h_ref[...], pw_ref[2], preferred_element_type=jnp.float32)
        values = values.astype(jnp.bfloat16)
        for branch in range(2):
            here = slice(branch * img, (branch + 1) * img)
            k_ref[branch, order * img : (order + 1) * img] = keys[here]
            v_ref[branch, order * img : (order + 1) * img] = values[here]
        if order == 0:
            found = jnp.dot(h_ref[...], pw_ref[0], preferred_element_type=jnp.float32)
            found = unit_heads(found, gain_ref[0:1], same_head, head_size)
            found = found * jnp.asarray(1.0 / math.sqrt(head_size), jnp.bfloat16)
            for branch in range(2):
                q_ref[branch] = found[branch * img : (branch + 1) * img]

    if size // 2 < 3:
        first.begin()
        second.begin()
    spread.ready(0)
    loads[3].wait()
    project(0)
    done = 1
    for step in range(2, size // 2 + 1):
        spread.advance(step)
        if step == size // 2 - 1:
            first.begin()
            second.begin()
        limit = len(spread.offsets) - (2 if step < size // 2 else 0)
        while done < limit:
            spread.relay(done)
            spread.ready(done)
            project(done)
            done += 1
    while done < len(spread.offsets):
        spread.relay(done)
        spread.ready(done)
        project(done)
        done += 1

    texts = ht_ref[...].reshape(-1, width)
    keys = jnp.dot(texts, pw_ref[3], preferred_element_type=jnp.float32)
    keys = unit_heads(keys, gain_ref[2:3], same_head, head_size)
    values = jnp.dot(texts, pw_ref[4], preferred_element_type=jnp.float32).astype(jnp.bfloat16)
    slots = size * sides * text
    for branch in range(2):
        kt_ref[branch] = keys[branch * slots : (branch + 1) * slots]
        vt_ref[branch] = values[branch * slots : (branch + 1) * slots]
    spot = lax.broadcasted_iota(jnp.int32, (1, slots), 1)
    within = lax.rem(spot, text)
    side_of = lax.rem(spot // text, sides)
    order_of = spot // (text * sides)
    block_of = jnp.zeros_like(spot)
    for order, offset in enumerate(spread.offsets):
        block_of = jnp.where(order_of == order, spread.at(offset), block_of)
    slot_of = (block_of * sides + side_of) * slot_count + within
    steps = first.order()

    chunk = img
    while chunk % 32 == 0 and 8 * chunk * k_ref.shape[1] > 2**20:
        chunk //= 2
    low = lax.broadcasted_iota(jnp.int32, (1, lanes), 1) < head_size
    loads[4].wait()
    partner = {"ulysses": row, "cfg": 1 - core}
    gift = pltpu.make_async_remote_copy(
        src_ref=give, dst_ref=got, send_sem=core_s, recv_sem=core_r,
        device_id=partner, device_id_type=MESH,
    )
    for turn in range(2):
        branch = 1 - core if turn == 0 else core
        limit = t_all[branch][:, time_cols : time_cols + 1].astype(jnp.int32)
        live = jnp.logical_and(slot_of < limit, within < slot_count)
        for left in range(0, inner, lanes):
            here = slice(left, left + lanes)

            def attend(step, carry, branch=branch, here=here, live=live):
                begin = step * chunk
                if chunk < img:
                    begin = pl.multiple_of(begin, chunk)
                queries = q_ref[branch, pl.ds(begin, chunk), here]
                nothing = jnp.zeros_like(queries)
                pair = jnp.concatenate(
                    [jnp.where(low, queries, nothing), jnp.where(low, nothing, queries)], axis=0
                )
                scores = lax.dot_general(
                    pair, k_ref[branch, :, here], flip, preferred_element_type=jnp.float32
                )
                words = lax.dot_general(
                    pair, kt_ref[branch, :, here], flip, preferred_element_type=jnp.float32
                )
                words = jnp.where(live, words, NEG_FILL)
                largest = jnp.maximum(
                    jnp.max(scores, axis=1, keepdims=True), jnp.max(words, axis=1, keepdims=True)
                )
                scores = jnp.exp(scores - largest)
                words = jnp.exp(words - largest)
                denominator = jnp.sum(scores, axis=1, keepdims=True)
                denominator = denominator + jnp.sum(words, axis=1, keepdims=True)
                update = jnp.dot(
                    scores.astype(jnp.bfloat16),
                    v_ref[branch, :, here],
                    preferred_element_type=jnp.float32,
                )
                update = update + jnp.dot(
                    words.astype(jnp.bfloat16),
                    vt_ref[branch, :, here],
                    preferred_element_type=jnp.float32,
                )
                update = update / denominator
                both = jnp.where(low, update[:chunk], update[chunk:]).astype(jnp.bfloat16)
                mix_ref[pl.ds(begin, chunk), here] = both
                return carry

            if chunk == img:
                attend(0, 0)
            else:
                lax.fori_loop(0, img // chunk, attend, 0)
        if turn == 0:
            out = jnp.dot(mix_ref[...], ow_ref[...], preferred_element_type=jnp.float32)
            give[...] = out.astype(jnp.bfloat16)
            gift.start()
            first.pass_on(steps[:2])

    def aside(step):
        return {"ulysses": lax.rem(row + step, sides), "cfg": core}

    def to_side(step):
        side = lax.rem(row + step, sides)
        return pltpu.make_async_remote_copy(
            src_ref=mine.at[side], dst_ref=att.at[row],
            send_sem=side_s.at[step], recv_sem=side_r.at[step],
            device_id=aside(step), device_id_type=MESH,
        )

    def from_side(step):
        side = lax.rem(row - step + sides, sides)
        return pltpu.make_async_remote_copy(
            src_ref=mine.at[side], dst_ref=att.at[side],
            send_sem=side_s.at[step], recv_sem=side_r.at[step],
            device_id=aside(step), device_id_type=MESH,
        )

    for step in list(range(1, sides)) + [0]:
        side = lax.rem(row + step, sides)
        start = pl.multiple_of(side * tokens, tokens)
        out = jnp.dot(
            mix_ref[pl.ds(start, tokens)], ow_ref[...], preferred_element_type=jnp.float32
        )
        if step == (1 if sides > 1 else 0):
            gift.wait_recv()
        out = out.astype(jnp.bfloat16).astype(jnp.float32)
        total = out + got[pl.ds(start, tokens)].astype(jnp.float32)
        if step:
            mine[side] = total.astype(jnp.bfloat16)
            to_side(step).start()
        else:
            att[row] = total.astype(jnp.bfloat16)
    first.pass_on(steps[2:])
    for step in range(1, sides):
        from_side(step).wait_recv()
    own_x = x_ref[...].astype(jnp.float32)
    own_x = jnp.concatenate([own_x[:rows], own_x[cut:]], axis=0)
    attended = att[0].astype(jnp.float32)
    for side in range(1, sides):
        attended = attended + att[side].astype(jnp.float32)
    residual = own_x + mod(core, 2) * attended
    res_ref[...] = residual
    feed_ref[...] = normed(residual, mod(core, 7), mod(core, 8))
    feed.own.start()
    feed.begin()
    second.pass_on(steps)
    gift.wait_send()
    for step in range(1, sides):
        to_side(step).wait_send()
    spread.end()

    depth = cfg["depth"]
    span = sides * tokens
    hidden = w1_ref.shape[1]
    share = w1_hbm.shape[1] // size
    begins = window(lax.axis_index("blk"), share, w1_hbm.shape[1], hidden)
    lane = begins + lax.broadcasted_iota(jnp.int32, (1, hidden), 1)
    base = lax.axis_index("blk") * share
    owned = jnp.logical_and(lane >= base, lane < base + share)

    def term_rows(slot, side_core):
        return pl.ds(pl.multiple_of((slot * 2 + side_core) * span, span), span)

    def give_copy(order):
        slot = order % depth
        return pltpu.make_async_remote_copy(
            src_ref=term.at[term_rows(slot, 1 - core)], dst_ref=gift_in.at[slot],
            send_sem=give_s.at[slot], recv_sem=give_r.at[slot],
            device_id=partner, device_id_type=MESH,
        )

    def over_copy(order, step, arriving):
        slot = order % depth
        side = lax.rem(row + step, sides)
        source = row
        if arriving:
            side = source = lax.rem(row - step + sides, sides)
        return pltpu.make_async_remote_copy(
            src_ref=x_out.at[slot, side], dst_ref=x_in.at[slot, source],
            send_sem=over_s.at[slot, step], recv_sem=over_r.at[slot, step],
            device_id=aside(step), device_id_type=MESH,
        )

    def line_copy(order):
        slot = order % depth
        return pltpu.make_async_remote_copy(
            src_ref=z_out.at[slot], dst_ref=z_in.at[order],
            send_sem=line_s.at[slot], recv_sem=line_r.at[order],
            device_id={"blk": feed.at(feed.offsets[order])}, device_id_type=MESH,
        )

    def expand(order):
        slot = order % depth
        if order >= depth:
            give_copy(order - depth).wait_send()
            pl.semaphore_wait(free_c, 1)
        where = feed.at(feed.offsets[order])
        if big:
            fetch = pltpu.make_async_copy(
                rows_ref.at[:, where], stage.at[:, pl.ds(0, tokens)], stage_s
            )
            fetch.start()
            fetch.wait()
            block = stage[:, :tokens]
        else:
            block = rows_ref[:, where]
        block = block.reshape(2 * span, width)
        pre = jnp.dot(block, w1_ref[...], preferred_element_type=jnp.float32)
        act = jnp.where(owned, jax.nn.gelu(pre, approximate=True), 0.0).astype(jnp.bfloat16)
        if order == 0:
            second.end()
        out = lax.dot_general(act, w2_ref[...], flip, preferred_element_type=jnp.float32)
        for side in range(sides):
            for half in range(2):
                start = ((slot * 2 + half) * sides + side) * tokens
                begin = (side * 2 + half) * tokens
                term[start : start + tokens] = out[begin : begin + tokens].astype(jnp.bfloat16)
        give_copy(order).start()

    def join(order):
        slot = order % depth
        if order >= depth:
            for step in range(1, sides):
                over_copy(order - depth, step, False).wait_send()
                pl.semaphore_wait(free_x.at[step], 1)
        give_copy(order).wait_recv()
        for step in list(range(1, sides)) + [0]:
            side = lax.rem(row + step, sides)
            start = pl.multiple_of(((slot * 2 + core) * sides + side) * tokens, tokens)
            near = pl.multiple_of(side * tokens, tokens)
            total = term[pl.ds(start, tokens)].astype(jnp.float32)
            total = total + gift_in[slot, pl.ds(near, tokens)].astype(jnp.float32)
            x_out[slot, side] = total.astype(jnp.bfloat16)
            if step:
                over_copy(order, step, False).start()
        if order + depth < size:
            pl.semaphore_signal(free_c, inc=1, device_id=partner, device_id_type=MESH)

    def settle(order):
        slot = order % depth
        if order > depth:
            line_copy(order - depth).wait_send()
        total = x_out[slot, row].astype(jnp.float32)
        for step in range(1, sides):
            over_copy(order, step, True).wait_recv()
            source = lax.rem(row - step + sides, sides)
            total = total + x_in[slot, source].astype(jnp.float32)
            if order + depth < size:
                pl.semaphore_signal(
                    free_x.at[step], inc=1,
                    device_id={"ulysses": source, "cfg": core}, device_id_type=MESH,
                )
        if order == 0:
            z_in[0] = total.astype(jnp.bfloat16)
        else:
            z_out[slot] = total.astype(jnp.bfloat16)
            line_copy(order).start()

    feed.relay(0)
    feed.advance(1)
    feed.ready(0)
    first.end()
    expand(0)
    done = 1

    def follow(order):
        feed.relay(order)
        feed.ready(order)
        expand(order)
        join(order - 1)
        if order > 1:
            settle(order - 2)

    for step in range(2, size // 2 + 1):
        feed.advance(step)
        limit = len(feed.offsets) - (2 if step < size // 2 else 0)
        while done < limit:
            follow(done)
            done += 1
    while done < len(feed.offsets):
        follow(done)
        done += 1
    settle(size - 2)
    join(size - 1)
    settle(size - 1)
    feed_out = z_in[0].astype(jnp.float32)
    for order in range(1, size):
        line_copy(order).wait_recv()
        feed_out = feed_out + z_in[order].astype(jnp.float32)
    ending = res_ref[...] + mod(core, 9) * feed_out
    ending = normed(ending, mod(core, 6), mod(core, 5))
    noise[...] = lax.dot_general(ending, fw_ref[...], flip, preferred_element_type=jnp.float32)
    swap = pltpu.make_async_remote_copy(
        src_ref=noise, dst_ref=noise_in, send_sem=last_s, recv_sem=last_r,
        device_id=partner, device_id_type=MESH,
    )
    swap.start()
    for order in range(size):
        if order + depth >= size:
            give_copy(order).wait_send()
            for step in range(1, sides):
                over_copy(order, step, False).wait_send()
            if order:
                line_copy(order).wait_send()
    feed.end()
    swap.wait()
    kept = noise[...]
    other = noise_in[...]
    cond = jnp.where(core == 0, kept, other)
    uncond = jnp.where(core == 0, other, kept)
    o_ref[...] = uncond + GUIDANCE * (cond - uncond)


def joint(
    sinusoid_rows, pooled, length, gains, packed, time_weight, time_second, mod_weight,
    proj_weight, out_weight, expand_weight, reduce_weight, final_weight, head_size, slot_count,
    rows, cut,
):
    axes = ("blk", "ulysses", "cfg")
    count = count_of(axes)
    size = lax.axis_size("blk")
    sides = lax.axis_size("ulysses")
    groups = lax.axis_size("groups")
    branches, width = pooled.shape
    inner = proj_weight.shape[2]
    tokens = 2 * rows
    img = sides * tokens
    text = cut - rows
    time_cols = time_second.shape[0]
    mod_cols = mod_weight.shape[0]
    padded = -(-(time_cols + 1) // LANES) * LANES
    quads = sides * 2
    all_shape = (quads, size) + packed.shape
    big = 2 * math.prod(all_shape) > 2**24
    parts = groups if expand_weight.shape[0] % (8 * groups) == 0 else 1
    hidden = expand_weight.shape[1]
    piece = window_width(hidden // size, hidden, size)
    peers = pltpu.SemaphoreType.DMA((count,))
    one = pltpu.SemaphoreType.DMA
    some = pltpu.SemaphoreType.DMA((sides,))
    vmem = pl.BlockSpec(memory_space=pltpu.VMEM)
    anywhere = pl.BlockSpec(memory_space=pl.ANY)
    bf16, f32 = jnp.bfloat16, jnp.float32
    sin_rows = jnp.broadcast_to(sinusoid_rows, (16, sinusoid_rows.shape[1]))
    pooled_rows = jnp.pad(pooled, ((0, 16 - branches), (0, 0)))
    depth = 2 if big else size
    needed = depth * 2 * sides * tokens
    reuse = mod_cols >= needed
    inputs = [sin_rows, pooled_rows, length, gains, packed, final_weight]
    inputs += [time_weight, time_second, mod_weight, proj_weight, out_weight, expand_weight, reduce_weight]
    feed_shape = (quads, size, tokens, width)
    outs = [jax.ShapeDtypeStruct((tokens, final_weight.shape[0]), f32)]
    gathers = [all_shape, feed_shape]
    if big:
        outs += [jax.ShapeDtypeStruct(shape, bf16) for shape in gathers]
    scratch = [] if big else [pltpu.VMEM(shape, bf16) for shape in gathers]
    scratch += [
        pltpu.VMEM((size * expand_weight.shape[0], piece), bf16),
        pltpu.VMEM((size * reduce_weight.shape[0], piece), bf16),
        pltpu.VMEM((tokens, width), f32),
        pltpu.VMEM((tokens, width), bf16),
        pltpu.VMEM((count, 1, padded), f32),
        pltpu.VMEM((count, branches, mod_cols), f32),
        pltpu.VMEM((branches, 1, count * mod_cols), f32),
        pltpu.VMEM(time_weight.shape, bf16),
        pltpu.VMEM(time_second.shape, bf16),
        pltpu.VMEM(mod_weight.shape, bf16),
        pltpu.VMEM(proj_weight.shape, bf16),
        pltpu.VMEM(out_weight.shape, bf16),
        pltpu.VMEM((quads,) + packed.shape if big else (1, 16, LANES), bf16),
        pltpu.VMEM((2 * img, width), bf16),
        pltpu.VMEM((2 * size * sides, text, width), bf16),
        pltpu.VMEM((2, img, inner), bf16),
        pltpu.VMEM((2, size * img, inner), bf16),
        pltpu.VMEM((2, size * img, inner), bf16),
        pltpu.VMEM((2, size * sides * text, inner), bf16),
        pltpu.VMEM((2, size * sides * text, inner), bf16),
        pltpu.VMEM((img, inner), bf16),
        pltpu.VMEM((img, width), bf16),
        pltpu.VMEM((img, width), bf16),
        pltpu.VMEM((sides, tokens, width), bf16),
        pltpu.VMEM((sides, tokens, width), bf16),
        pltpu.VMEM((16, LANES) if reuse else (needed, width), bf16),
        pltpu.VMEM((depth, img, width), bf16),
        pltpu.VMEM((depth, sides, tokens, width), bf16),
        pltpu.VMEM((depth, sides, tokens, width), bf16),
        pltpu.VMEM((depth, tokens, width), bf16),
        pltpu.VMEM((size, tokens, width), bf16),
        pltpu.VMEM((tokens, final_weight.shape[0]), f32),
        pltpu.VMEM((tokens, final_weight.shape[0]), f32),
        pltpu.SemaphoreType.DMA((5,)),
        peers, peers, peers, peers, one, one, some, some, one,
        pltpu.SemaphoreType.DMA((depth,)),
        pltpu.SemaphoreType.DMA((depth,)),
        pltpu.SemaphoreType.DMA((depth, sides)),
        pltpu.SemaphoreType.DMA((depth, sides)),
        pltpu.SemaphoreType.DMA((depth,)),
        pltpu.SemaphoreType.DMA((size,)),
        one, one,
        pltpu.SemaphoreType.REGULAR,
        pltpu.SemaphoreType.REGULAR((sides,)),
    ]
    cfg = dict(
        count=len(inputs) + len(outs) + len(scratch), head_size=head_size, slot_count=slot_count,
        rows=rows, cut=cut, big=big, parts=parts,
        depth=depth, reuse=reuse,
    )
    return pl.pallas_call(
        functools.partial(joint_kernel, cfg),
        out_shape=outs,
        in_specs=[vmem] * 6 + [anywhere] * 7,
        out_specs=[vmem] + [anywhere] * (len(outs) - 1),
        scratch_shapes=scratch
        + spread_sems()
        + shuffle_sems(parts)
        + shuffle_sems(parts)
        + spread_sems(),
        compiler_params=pltpu.CompilerParams(
            collective_id=0, has_side_effects=True, vmem_limit_bytes=63 * 2**20
        ),
        name="joint",
    )(*inputs)[0]


def body(
    img_tokens,
    text_tokens,
    text_lengths,
    timestep,
    pooled,
    time_weight,
    time_second,
    mod_weight,
    proj_weight,
    out_weight,
    expand_weight,
    reduce_weight,
    qk_gain,
    final_weight,
):
    model_width = img_tokens.shape[3]
    branches = pooled.shape[0]
    head_size = qk_gain.shape[1]
    token_count = img_tokens.shape[2]
    slot_count = text_tokens.shape[2]
    rows = token_count // 2
    text_pad = -(-slot_count // 8) * 8
    image = img_tokens[0, 0]
    text = jnp.pad(text_tokens[0, 0], ((0, text_pad - slot_count), (0, 0)))
    packed = jnp.concatenate([image[:rows], text, image[rows:]], axis=0)
    guided = joint(
        sinusoid(timestep, time_weight.shape[0]).astype(jnp.bfloat16),
        pooled.reshape(branches, model_width),
        text_lengths.astype(jnp.float32),
        jnp.tile(qk_gain, (1, proj_weight.shape[2] // head_size)),
        packed,
        time_weight,
        time_second.T,
        mod_weight.T,
        proj_weight,
        out_weight,
        expand_weight,
        reduce_weight.T,
        final_weight.T,
        head_size,
        slot_count,
        rows,
        rows + text_pad,
    )
    channels = final_weight.shape[1] // 4
    guided = guided.reshape(token_count, 2, 2, channels)
    kept = lax.dynamic_index_in_dim(guided, lax.axis_index("cfg"), 1, keepdims=False)
    return kept.transpose(2, 0, 1).reshape(1, channels, 1, 2 * token_count)


def solution(mesh):
    in_specs = (
        P("cfg", "groups", ("blk", "ulysses"), None),
        P("cfg", "groups", ("blk", "ulysses"), None),
        P("cfg", "groups"),
        P("groups"),
        P(None, "groups", None),
        P(),
        P(None, ("blk", "ulysses", "cfg")),
        P(None, ("blk", "ulysses", "cfg")),
        P(None, None, ("ulysses", "cfg")),
        P(("ulysses", "cfg"), None),
        P("blk", ("ulysses", "cfg")),
        P(("ulysses", "cfg"), "blk"),
        P(),
        P(),
    )
    out_specs = P("groups", None, ("blk", "ulysses", "cfg"), None)
    return jax.shard_map(body, mesh=mesh, in_specs=in_specs, out_specs=out_specs, check_vma=False)
```

```python
import functools
import math

import jax
import jax.numpy as jnp
from jax import lax
from jax.experimental import pallas as pl
from jax.experimental.pallas import tpu as pltpu
from jax.sharding import PartitionSpec as P

GUIDANCE = 3.5
LN_EPS = 1e-06
RMS_EPS = 1e-06
NEG_FILL = -1e30
LANES = 128
MESH = pl.DeviceIdType.MESH


def sinusoid(timestep, feature_count):
    half_width = feature_count // 2
    frequency = jnp.exp(-math.log(10000.0) * jnp.arange(half_width, dtype=jnp.float32) / half_width)
    angles = timestep.astype(jnp.float32)[:, None] * frequency[None, :]
    return jnp.concatenate([jnp.cos(angles), jnp.sin(angles)], axis=1)


def silu(value):
    return value / (1.0 + jnp.exp(-value))


def flat_position(axes):
    position = 0
    for axis in axes:
        position = position * lax.axis_size(axis) + lax.axis_index(axis)
    return position


def coordinates(position, axes):
    found = {}
    for axis in reversed(axes):
        size = lax.axis_size(axis)
        found[axis] = lax.rem(position, size)
        position = position // size
    return found


def count_of(axes):
    return math.prod(lax.axis_size(axis) for axis in axes)


def normed(values, shift, scale):
    average = jnp.mean(values, axis=-1, keepdims=True)
    centred = values - average
    variance = jnp.mean(centred * centred, axis=-1, keepdims=True)
    return (centred * lax.rsqrt(variance + LN_EPS) * (1.0 + scale) + shift).astype(jnp.bfloat16)


def unit_heads(values, gains, same_head, head_size):
    parts = []
    lanes = same_head.shape[0]
    for first in range(0, values.shape[1], lanes):
        piece = values[:, first : first + lanes]
        square = piece * piece
        high = square.astype(jnp.bfloat16)
        low = (square - high.astype(jnp.float32)).astype(jnp.bfloat16)
        total = jnp.dot(high, same_head, preferred_element_type=jnp.float32)
        total = total + jnp.dot(low, same_head, preferred_element_type=jnp.float32)
        scale = lax.rsqrt(total * (1.0 / head_size) + RMS_EPS)
        parts.append((piece * scale * gains[:, first : first + lanes]).astype(jnp.bfloat16))
    return jnp.concatenate(parts, axis=1)


def window(index, share, total, width):
    start = jnp.minimum(index * share // LANES * LANES, total - width)
    return pl.multiple_of(start, LANES)


def window_width(share, total, parts):
    ends = [-(-(index + 1) * share // LANES) - index * share // LANES for index in range(parts)]
    return min(max(ends) * LANES, total)


class Spread:
    def __init__(self, x_ref, o_ref, cut, sems):
        self.x_ref, self.o_ref, self.cut = x_ref, o_ref, cut
        self.hop_s, self.hop_r, self.x_s, self.x_r = sems[:4]
        self.c_s, self.c_r, self.f_s, self.f_r = sems[4:8]
        self.local = sems[8]
        self.size = lax.axis_size("blk")
        self.me = lax.axis_index("blk")
        self.last = self.size // 2
        self.halved = self.size % 2 == 0
        self.sides = lax.axis_size("ulysses")
        self.row = lax.axis_index("ulysses")
        self.core = lax.axis_index("cfg")
        self.partner = {"ulysses": self.row, "cfg": 1 - self.core}
        self.base = o_ref.at[self.row * 2 + self.core]
        self.offsets = [0]
        self.sent = []
        self.own = pltpu.make_async_copy(x_ref, self.base.at[self.me], self.local)

    def at(self, offset):
        return lax.rem(self.me + offset + self.size, self.size)

    def copy(self, source, target, send, recv, device):
        return pltpu.make_async_remote_copy(
            src_ref=source,
            dst_ref=target,
            send_sem=send,
            recv_sem=recv,
            device_id=device,
            device_id_type=MESH,
        )

    def part(self, ref, way, step):
        if self.halved and step == self.last:
            rows = ref.shape[0]
            return ref.at[pl.ds(0, self.cut)] if way == 1 else ref.at[pl.ds(self.cut, rows - self.cut)]
        return ref

    def hop(self, way, step):
        slot = self.at(-way * (step - 1))
        source = self.x_ref if step == 1 else self.base.at[slot]
        sem = ((way + 1) // 2, step)
        return self.copy(
            self.part(source, way, step),
            self.part(self.base.at[slot], way, step),
            self.hop_s.at[sem],
            self.hop_r.at[sem],
            {"blk": self.at(way)},
        )

    def hop_in(self, way, step):
        slot = self.part(self.base.at[self.at(-way * step)], way, step)
        sem = ((way + 1) // 2, step)
        return self.copy(
            slot, slot, self.hop_s.at[sem], self.hop_r.at[sem], {"blk": self.at(-way)}
        )

    def aside(self, step):
        return {"ulysses": lax.rem(self.row + step, self.sides), "cfg": self.core}

    def send(self, order, step):
        slot = self.at(self.offsets[order])
        return self.copy(
            self.x_ref if order == 0 else self.base.at[slot],
            self.base.at[slot],
            self.x_s.at[order, step] if step else self.c_s.at[order],
            self.x_r.at[order, step] if step else self.c_r.at[order],
            self.aside(step) if step else self.partner,
        )

    def across_in(self, order, step):
        source = lax.rem(self.row - step + self.sides, self.sides)
        block = self.o_ref.at[source * 2 + self.core, self.at(self.offsets[order])]
        return self.copy(
            block, block, self.x_s.at[order, step], self.x_r.at[order, step], self.aside(step)
        )

    def forward(self, order, step, side):
        source = lax.rem(self.row - step + self.sides, self.sides)
        block = self.o_ref.at[source * 2 + side, self.at(self.offsets[order])]
        return self.copy(
            block, block, self.f_s.at[order, step], self.f_r.at[order, step], self.partner
        )

    def beside_in(self, order):
        block = self.o_ref.at[self.row * 2 + 1 - self.core, self.at(self.offsets[order])]
        return self.copy(block, block, self.c_s.at[order], self.c_r.at[order], self.partner)

    def pass_on(self, order):
        for step in list(range(1, self.sides)) + [0]:
            self.send(order, step).start()

    def begin(self):
        for way in (1, -1):
            self.hop(way, 1).start()
        self.pass_on(0)

    def advance(self, step):
        final = self.halved and step == self.last
        for way in (1, -1):
            self.hop_in(way, step).wait_recv()
            if step < self.last:
                self.hop(way, step + 1).start()
            if not final:
                self.offsets.append(-way * step)
                self.pass_on(len(self.offsets) - 1)
        if final:
            self.offsets.append(step)
            self.pass_on(len(self.offsets) - 1)

    def relay(self, order):
        for step in range(1, self.sides):
            self.across_in(order, step).wait_recv()
            self.forward(order, step, self.core).start()

    def ready(self, order):
        for step in range(1, self.sides):
            self.forward(order, step, 1 - self.core).wait_recv()
        self.beside_in(order).wait_recv()
        if order == 0:
            self.own.wait()

    def end(self):
        for step in range(1, self.last + 1):
            for way in (1, -1):
                self.hop(way, step).wait_send()
        for order in range(len(self.offsets)):
            for step in range(self.sides):
                self.send(order, step).wait_send()
            for step in range(1, self.sides):
                self.forward(order, step, self.core).wait_send()


def spread_sems():
    size = lax.axis_size("blk")
    hops = pltpu.SemaphoreType.DMA((2, size // 2 + 1))
    across = pltpu.SemaphoreType.DMA((size, lax.axis_size("ulysses")))
    beside = pltpu.SemaphoreType.DMA((size,))
    one = pltpu.SemaphoreType.DMA
    return [hops, hops, across, across, beside, beside, across, across, one]


def greet_all():
    axes = ("blk", "ulysses", "cfg")
    count = count_of(axes)
    place = flat_position(axes)
    groups = lax.axis_size("groups")
    barrier = pltpu.get_barrier_semaphore()

    def greet(step, carry):
        pl.semaphore_signal(
            barrier,
            inc=1,
            device_id=coordinates(lax.rem(place + step, count), axes),
            device_id_type=MESH,
        )
        return carry

    lax.fori_loop(1, count, greet, 0)
    for step in range(1, groups):
        other = lax.rem(lax.axis_index("groups") + step, groups)
        pl.semaphore_signal(barrier, inc=1, device_id={"groups": other}, device_id_type=MESH)
    return barrier, count - 1 + groups - 1


class Shuffle:
    def __init__(self, source, target, sems, parts):
        self.source, self.target, self.parts = source, target, parts
        self.z_s, self.z_r, self.y_s, self.y_r, self.local = sems
        self.size = lax.axis_size("blk")
        self.me = lax.axis_index("blk")
        self.part = lax.axis_index("groups")
        self.rows, self.total = source.shape
        self.share = self.total // self.size
        self.width = target.shape[1]
        self.height = self.rows // parts

    def columns(self, index):
        return pl.ds(window(index, self.share, self.total, self.width), self.width)

    def block(self, index, part):
        start = index * self.rows
        if self.parts > 1:
            start = start + part * self.height
        return self.target.at[pl.ds(pl.multiple_of(start, 8), self.height)]

    def piece(self, index):
        if self.parts == 1:
            return self.source.at[:, self.columns(index)]
        start = pl.multiple_of(self.part * self.height, 8)
        return self.source.at[pl.ds(start, self.height), self.columns(index)]

    def own(self):
        start = pl.multiple_of(self.me * self.rows, 8)
        return pltpu.make_async_copy(
            self.source.at[:, self.columns(self.me)],
            self.target.at[pl.ds(start, self.rows)],
            self.local,
        )

    def remote(self, source, target, send, recv, device):
        return pltpu.make_async_remote_copy(
            src_ref=source,
            dst_ref=target,
            send_sem=send,
            recv_sem=recv,
            device_id=device,
            device_id_type=MESH,
        )

    def out(self, step):
        target = lax.rem(self.me + step, self.size)
        return self.remote(
            self.piece(target),
            self.block(self.me, self.part),
            self.z_s.at[step],
            self.z_r.at[step],
            {"blk": target},
        )

    def into(self, step):
        source = lax.rem(self.me - step + self.size, self.size)
        return self.remote(
            self.block(source, self.part),
            self.block(source, self.part),
            self.z_s.at[step],
            self.z_r.at[step],
            {"blk": source},
        )

    def cross(self, step, turn, arriving):
        origin = lax.rem(self.me - step + self.size, self.size)
        part = self.part
        other = lax.rem(self.part + turn, self.parts)
        if arriving:
            part = other = lax.rem(self.part - turn + self.parts, self.parts)
        block = self.block(origin, part)
        return self.remote(
            block, block, self.y_s.at[step, turn], self.y_r.at[step, turn], {"groups": other}
        )

    def begin(self, steps):
        for step in steps:
            self.out(step).start()

    def order(self):
        half = self.size // 2
        steps = [half] if self.size > 1 else []
        for step in range(1, half + 1):
            steps += [near for near in (half - step, half + step) if 0 < near < self.size]
        return steps

    def pass_on(self, steps):
        for step in steps:
            self.into(step).wait_recv()
            for turn in range(1, self.parts):
                self.cross(step, turn, False).start()

    def complete(self, step):
        for turn in range(1, self.parts):
            self.cross(step, turn, True).wait_recv()

    def end(self):
        for step in self.order():
            self.out(step).wait_send()
            for turn in range(1, self.parts):
                self.cross(step, turn, False).wait_send()


def shuffle_sems(parts):
    size = lax.axis_size("blk")
    line = pltpu.SemaphoreType.DMA((size,))
    grid = pltpu.SemaphoreType.DMA((size, max(parts, 2)))
    return [line, line, grid, grid, pltpu.SemaphoreType.DMA]


def joint_kernel(cfg, *refs):
    (
        sin_ref, pooled_ref, len_ref, gains_ref, img_ref, text_ref,
        fw_ref, tw_hbm, ts_hbm, mw_hbm, pw_hbm, ow_hbm, w1_hbm, w2_hbm,
        o_ref, tok_ref, rows_ref, x_ref, w1_ref, w2_ref, res_ref, feed_ref,
        t_all, m_all, mod_ref, tw_ref, ts_ref, mw_ref, pw_ref, ow_ref,
        stage, h_ref, ht_ref, q_ref, k_ref, v_ref, kt_ref, vt_ref, mix_ref,
        give, got, mine, att, term, gift_in, x_out, x_in, z_out, z_in, noise, noise_in, act_ref,
        load_s, t_s, t_r, m_s, m_r, core_s, core_r, side_s, side_r, stage_s,
        give_s, give_r, over_s, over_r, line_s, line_r, last_s, last_r, free_c, free_x,
    ) = refs[: cfg["count"]]
    sems = list(refs[cfg["count"] :])
    head_size, slot_count = cfg["head_size"], cfg["slot_count"]
    rows, cut, big = cfg["rows"], cfg["cut"], cfg["big"]
    axes = ("blk", "ulysses", "cfg")
    count = count_of(axes)
    place = flat_position(axes)
    size = lax.axis_size("blk")
    sides = lax.axis_size("ulysses")
    row = lax.axis_index("ulysses")
    core = lax.axis_index("cfg")
    width = x_ref.shape[1]
    gain_ref = jnp.concatenate([gains_ref[...]] * (pw_ref.shape[2] // head_size), axis=1)
    inner = pw_ref.shape[2]
    tokens = 2 * rows
    img = sides * tokens
    text = cut - rows
    time_cols = ts_ref.shape[0]
    lanes = 2 * head_size

    loads = [
        pltpu.make_async_copy(source, target, load_s.at[index])
        for index, (source, target) in enumerate(
            [(tw_hbm, tw_ref), (ts_hbm, ts_ref), (mw_hbm, mw_ref), (pw_hbm, pw_ref), (ow_hbm, ow_ref)]
        )
    ]
    for load in loads:
        load.start()
    spread = Spread(x_ref, tok_ref, cut, sems[:9])
    first = Shuffle(w1_hbm, w1_ref, sems[9:14], cfg["parts"])
    second = Shuffle(w2_hbm, w2_ref, sems[14:19], cfg["parts"])
    feed = Spread(feed_ref, rows_ref, rows, sems[19:28])
    if cfg["reuse"]:
        term = mw_ref
    barrier, expected = greet_all()
    x_ref[:rows] = img_ref[:rows]
    x_ref[cut:] = img_ref[rows:]
    words = [text_ref[...]]
    if text > slot_count:
        words.append(jnp.zeros((text - slot_count, width), jnp.bfloat16))
    x_ref[rows:cut] = jnp.concatenate(words, axis=0)

    def outgoing(ref, send, recv, step):
        return pltpu.make_async_remote_copy(
            src_ref=ref.at[place],
            dst_ref=ref.at[place],
            send_sem=send.at[step],
            recv_sem=recv.at[step],
            device_id=coordinates(lax.rem(place + step, count), axes),
            device_id_type=MESH,
        )

    def incoming(ref, send, recv, step):
        source = lax.rem(place - step + count, count)
        return pltpu.make_async_remote_copy(
            src_ref=ref.at[source],
            dst_ref=ref.at[source],
            send_sem=send.at[step],
            recv_sem=recv.at[step],
            device_id=coordinates(source, axes),
            device_id_type=MESH,
        )

    def send_all(ref, send, recv):
        def begin(step, carry):
            outgoing(ref, send, recv, step).start()
            return carry

        lax.fori_loop(1, count, begin, 0)

    def wait_all(ref, send, recv):
        def finish(step, carry):
            incoming(ref, send, recv, step).wait_recv()
            outgoing(ref, send, recv, step).wait_send()
            return carry

        lax.fori_loop(1, count, finish, 0)

    flip = (((1,), (1,)), ((), ()))
    loads[0].wait()
    sin_rows = jnp.broadcast_to(sin_ref[...], (16, sin_ref.shape[1]))
    hidden = jnp.dot(sin_rows, tw_ref[...], preferred_element_type=jnp.float32)
    hidden = silu(hidden).astype(jnp.bfloat16)
    loads[1].wait()
    part = lax.dot_general(hidden, ts_ref[...], flip, preferred_element_type=jnp.float32)[0:1]
    length = jnp.broadcast_to(len_ref[...], (1, t_all.shape[2] - time_cols))
    t_all[place] = jnp.concatenate([part, length], axis=1)
    pl.semaphore_wait(barrier, expected)
    send_all(t_all, t_s, t_r)
    spread.own.start()
    spread.begin()
    wait_all(t_all, t_s, t_r)
    embed = jnp.concatenate([t_all[i][:, :time_cols] for i in range(count)], axis=1)
    acted = [silu(embed + pooled_ref[branch]) for branch in range(2)]
    acted = jnp.concatenate(acted + [jnp.zeros((14, width), jnp.float32)], axis=0)
    acted = acted.astype(jnp.bfloat16)
    loads[2].wait()
    mods = lax.dot_general(acted, mw_ref[...], flip, preferred_element_type=jnp.float32)
    m_all[place] = mods[0:2]
    send_all(m_all, m_s, m_r)
    spread.advance(1)
    spread.relay(0)
    wait_all(m_all, m_s, m_r)
    for branch in range(2):
        mod_ref[branch] = jnp.concatenate(
            [m_all[i][branch : branch + 1] for i in range(count)], axis=1
        )

    def mod(branch, index):
        return mod_ref[branch, :, index * width : (index + 1) * width]

    head_row = lax.broadcasted_iota(jnp.int32, (lanes, lanes), 0) // head_size
    head_col = lax.broadcasted_iota(jnp.int32, (lanes, lanes), 1) // head_size
    same_head = jnp.where(head_row == head_col, 1.0, 0.0).astype(jnp.bfloat16)

    steps = first.order()
    early = steps[: (len(steps) + 2) // 3]
    late = steps[len(early) :]

    def start_weights():
        first.own().start()
        second.own().start()
        first.begin(steps)
        second.begin(early)

    def project(order):
        slot = spread.at(spread.offsets[order])
        if big:
            fetch = pltpu.make_async_copy(tok_ref.at[:, slot], stage, stage_s)
            fetch.start()
            fetch.wait()

        def tile(side, branch):
            index = side * 2 + branch
            return stage[index] if big else tok_ref[index, slot]

        for branch in range(2):
            for side in range(sides):
                x = tile(side, branch).astype(jnp.float32)
                start = branch * img + side * tokens
                h_ref[start : start + rows] = normed(x[:rows], mod(branch, 0), mod(branch, 1))
                h_ref[start + rows : start + tokens] = normed(
                    x[cut:], mod(branch, 0), mod(branch, 1)
                )
                spot = (branch * size + order) * sides + side
                ht_ref[spot] = normed(x[rows:cut], mod(branch, 4), mod(branch, 3))
        keys = jnp.dot(h_ref[...], pw_ref[1], preferred_element_type=jnp.float32)
        keys = unit_heads(keys, gain_ref[1:2], same_head, head_size)
        values = jnp.dot(h_ref[...], pw_ref[2], preferred_element_type=jnp.float32)
        values = values.astype(jnp.bfloat16)
        for branch in range(2):
            here = slice(branch * img, (branch + 1) * img)
            k_ref[branch, order * img : (order + 1) * img] = keys[here]
            v_ref[branch, order * img : (order + 1) * img] = values[here]
        if order == 0:
            found = jnp.dot(h_ref[...], pw_ref[0], preferred_element_type=jnp.float32)
            found = unit_heads(found, gain_ref[0:1], same_head, head_size)
            found = found * jnp.asarray(1.0 / math.sqrt(head_size), jnp.bfloat16)
            for branch in range(2):
                q_ref[branch] = found[branch * img : (branch + 1) * img]

    if size // 2 < 3:
        start_weights()
    spread.ready(0)
    loads[3].wait()
    project(0)
    done = 1
    for step in range(2, size // 2 + 1):
        spread.advance(step)
        if step == size // 2 - 1:
            start_weights()
        limit = len(spread.offsets) - (2 if step < size // 2 else 0)
        while done < limit:
            spread.relay(done)
            spread.ready(done)
            project(done)
            done += 1
    while done < len(spread.offsets):
        spread.relay(done)
        spread.ready(done)
        project(done)
        done += 1

    texts = ht_ref[...].reshape(-1, width)
    keys = jnp.dot(texts, pw_ref[3], preferred_element_type=jnp.float32)
    keys = unit_heads(keys, gain_ref[2:3], same_head, head_size)
    values = jnp.dot(texts, pw_ref[4], preferred_element_type=jnp.float32).astype(jnp.bfloat16)
    slots = size * sides * text
    for branch in range(2):
        kt_ref[branch] = keys[branch * slots : (branch + 1) * slots]
        vt_ref[branch] = values[branch * slots : (branch + 1) * slots]
    spot = lax.broadcasted_iota(jnp.int32, (1, slots), 1)
    within = lax.rem(spot, text)
    side_of = lax.rem(spot // text, sides)
    order_of = spot // (text * sides)
    block_of = jnp.zeros_like(spot)
    for order, offset in enumerate(spread.offsets):
        block_of = jnp.where(order_of == order, spread.at(offset), block_of)
    slot_of = (block_of * sides + side_of) * slot_count + within
    chunk = img
    while chunk % 32 == 0 and 8 * chunk * k_ref.shape[1] > 2**20:
        chunk //= 2
    low = lax.broadcasted_iota(jnp.int32, (1, lanes), 1) < head_size
    loads[4].wait()
    partner = {"ulysses": row, "cfg": 1 - core}
    gift = pltpu.make_async_remote_copy(
        src_ref=give, dst_ref=got, send_sem=core_s, recv_sem=core_r,
        device_id=partner, device_id_type=MESH,
    )
    for turn in range(2):
        branch = 1 - core if turn == 0 else core
        limit = t_all[branch][:, time_cols : time_cols + 1].astype(jnp.int32)
        live = jnp.logical_and(slot_of < limit, within < slot_count)
        for left in range(0, inner, lanes):
            here = slice(left, left + lanes)

            def attend(step, carry, branch=branch, here=here, live=live):
                begin = step * chunk
                if chunk < img:
                    begin = pl.multiple_of(begin, chunk)
                queries = q_ref[branch, pl.ds(begin, chunk), here]
                nothing = jnp.zeros_like(queries)
                pair = jnp.concatenate(
                    [jnp.where(low, queries, nothing), jnp.where(low, nothing, queries)], axis=0
                )
                scores = lax.dot_general(
                    pair, k_ref[branch, :, here], flip, preferred_element_type=jnp.float32
                )
                words = lax.dot_general(
                    pair, kt_ref[branch, :, here], flip, preferred_element_type=jnp.float32
                )
                words = jnp.where(live, words, NEG_FILL)
                largest = jnp.maximum(
                    jnp.max(scores, axis=1, keepdims=True), jnp.max(words, axis=1, keepdims=True)
                )
                scores = jnp.exp(scores - largest)
                words = jnp.exp(words - largest)
                denominator = jnp.sum(scores, axis=1, keepdims=True)
                denominator = denominator + jnp.sum(words, axis=1, keepdims=True)
                update = jnp.dot(
                    scores.astype(jnp.bfloat16),
                    v_ref[branch, :, here],
                    preferred_element_type=jnp.float32,
                )
                update = update + jnp.dot(
                    words.astype(jnp.bfloat16),
                    vt_ref[branch, :, here],
                    preferred_element_type=jnp.float32,
                )
                update = update / denominator
                both = jnp.where(low, update[:chunk], update[chunk:]).astype(jnp.bfloat16)
                mix_ref[pl.ds(begin, chunk), here] = both
                return carry

            if chunk == img:
                attend(0, 0)
            else:
                lax.fori_loop(0, img // chunk, attend, 0)
        if turn == 0:
            out = jnp.dot(mix_ref[...], ow_ref[...], preferred_element_type=jnp.float32)
            give[...] = out.astype(jnp.bfloat16)
            gift.start()

    def aside(step):
        return {"ulysses": lax.rem(row + step, sides), "cfg": core}

    def to_side(step):
        side = lax.rem(row + step, sides)
        return pltpu.make_async_remote_copy(
            src_ref=mine.at[side], dst_ref=att.at[row],
            send_sem=side_s.at[step], recv_sem=side_r.at[step],
            device_id=aside(step), device_id_type=MESH,
        )

    def from_side(step):
        side = lax.rem(row - step + sides, sides)
        return pltpu.make_async_remote_copy(
            src_ref=mine.at[side], dst_ref=att.at[side],
            send_sem=side_s.at[step], recv_sem=side_r.at[step],
            device_id=aside(step), device_id_type=MESH,
        )

    for step in list(range(1, sides)) + [0]:
        side = lax.rem(row + step, sides)
        start = pl.multiple_of(side * tokens, tokens)
        out = jnp.dot(
            mix_ref[pl.ds(start, tokens)], ow_ref[...], preferred_element_type=jnp.float32
        )
        if step == (1 if sides > 1 else 0):
            gift.wait_recv()
        out = out.astype(jnp.bfloat16).astype(jnp.float32)
        total = out + got[pl.ds(start, tokens)].astype(jnp.float32)
        if step:
            mine[side] = total.astype(jnp.bfloat16)
            to_side(step).start()
        else:
            att[row] = total.astype(jnp.bfloat16)
    for step in range(1, sides):
        from_side(step).wait_recv()
    own_x = img_ref[...].astype(jnp.float32)
    attended = att[0].astype(jnp.float32)
    for side in range(1, sides):
        attended = attended + att[side].astype(jnp.float32)
    residual = own_x + mod(core, 2) * attended
    res_ref[...] = residual
    feed_ref[...] = normed(residual, mod(core, 7), mod(core, 8))
    feed.own.start()
    feed.begin()
    first.pass_on(steps)
    second.pass_on(early)
    gift.wait_send()
    for step in range(1, sides):
        to_side(step).wait_send()
    spread.end()

    depth, groups = cfg["depth"], cfg["groups"]
    span = sides * tokens
    cols = width // groups
    padded = z_in.shape[3]
    hidden = w1_ref.shape[1]
    share = w1_hbm.shape[1] // size
    begins = window(lax.axis_index("blk"), share, w1_hbm.shape[1], hidden)
    lane = begins + lax.broadcasted_iota(jnp.int32, (1, hidden), 1)
    base = lax.axis_index("blk") * share
    owned = jnp.logical_and(lane >= base, lane < base + share)
    pieces = [0] + steps

    def column(piece, source):
        return lax.rem(source - pieces[piece] + size, size) if groups > 1 else 0

    def term_at(piece, slot):
        if not cfg["reuse"]:
            return term.at[slot]
        unit = piece * depth + slot
        strips = width // padded
        return term.at[
            pl.ds(unit // strips * span, span), pl.ds(unit % strips * padded, padded)
        ]

    def give_copy(piece, order):
        slot = order % depth
        return pltpu.make_async_remote_copy(
            src_ref=term_at(piece, slot), dst_ref=gift_in.at[piece, slot],
            send_sem=give_s.at[piece, slot], recv_sem=give_r.at[piece, slot],
            device_id=partner, device_id_type=MESH,
        )

    def over_copy(piece, order, step, arriving):
        slot = order % depth
        side = lax.rem(row + step, sides)
        source = row
        if arriving:
            side = source = lax.rem(row - step + sides, sides)
        return pltpu.make_async_remote_copy(
            src_ref=x_out.at[piece, slot, side], dst_ref=x_in.at[piece, slot, source],
            send_sem=over_s.at[piece, slot, step], recv_sem=over_r.at[piece, slot, step],
            device_id=aside(step), device_id_type=MESH,
        )

    def line_copy(piece, order, arriving=False):
        slot = order % depth
        offset = feed.offsets[order]
        source = feed.at(-offset) if arriving else feed.me
        return pltpu.make_async_remote_copy(
            src_ref=z_out.at[piece, slot], dst_ref=z_in.at[column(piece, source), order],
            send_sem=line_s.at[piece, slot], recv_sem=line_r.at[piece, order],
            device_id={"blk": feed.at(-offset if arriving else offset)}, device_id_type=MESH,
        )

    def expand(order):
        where = feed.at(feed.offsets[order])
        if big:
            fetch = pltpu.make_async_copy(
                rows_ref.at[:, where], stage.at[:, pl.ds(0, tokens)], stage_s
            )
            fetch.start()
            fetch.wait()

        def rows_of(index):
            return stage[index, :tokens] if big else rows_ref[index, where]

        block = [rows_of(side * 2 + core) for side in range(sides)]
        block += [rows_of(side * 2 + 1 - core) for side in range(sides)]
        block = jnp.concatenate(block, axis=0)
        pre = jnp.dot(block, w1_ref[...], preferred_element_type=jnp.float32)
        act = jnp.where(owned, jax.nn.gelu(pre, approximate=True), 0.0)
        act_ref[0 if big else order] = act.astype(jnp.bfloat16)

    def shrink(piece, order):
        slot = order % depth
        if order >= depth:
            give_copy(piece, order - depth).wait_send()
            for step in range(1, sides):
                over_copy(piece, order - depth, step, False).wait_send()
            pl.semaphore_wait(free_c, 1)
        act = act_ref[0 if big else order]
        if groups > 1:
            start = pl.multiple_of(column(piece, feed.me) * cols, 8)
            weight = w2_ref[pl.ds(start, cols)]
        else:
            weight = w2_ref[...]
        out = lax.dot_general(act, weight, flip, preferred_element_type=jnp.float32)
        if padded > cols:
            out = jnp.concatenate(
                [out, jnp.zeros((out.shape[0], padded - cols), jnp.float32)], axis=1
            )
        out = out.astype(jnp.bfloat16)
        if cfg["reuse"]:
            unit = piece * depth + slot
            strips = width // padded
            high, left = unit // strips * span, unit % strips * padded
            term[high : high + span, left : left + padded] = out[span:]
        else:
            term[slot] = out[span:]
        give_copy(piece, order).start()
        for side in range(sides):
            x_out[piece, slot, side] = out[side * tokens : (side + 1) * tokens]

    def join(piece, order):
        slot = order % depth
        if order >= depth:
            for step in range(1, sides):
                pl.semaphore_wait(free_x.at[step], 1)
        give_copy(piece, order).wait_recv()
        for step in list(range(1, sides)) + [0]:
            side = lax.rem(row + step, sides)
            near = pl.multiple_of(side * tokens, tokens)
            total = x_out[piece, slot, side].astype(jnp.float32)
            total = total + gift_in[piece, slot, pl.ds(near, tokens)].astype(jnp.float32)
            x_out[piece, slot, side] = total.astype(jnp.bfloat16)
            if step:
                over_copy(piece, order, step, False).start()
        if order + depth < size:
            pl.semaphore_signal(free_c, inc=1, device_id=partner, device_id_type=MESH)

    def settle(piece, order):
        slot = order % depth
        if order > depth:
            line_copy(piece, order - depth).wait_send()
        total = x_out[piece, slot, row].astype(jnp.float32)
        for step in range(1, sides):
            over_copy(piece, order, step, True).wait_recv()
            source = lax.rem(row - step + sides, sides)
            total = total + x_in[piece, slot, source].astype(jnp.float32)
            if order + depth < size:
                pl.semaphore_signal(
                    free_x.at[step], inc=1,
                    device_id={"ulysses": source, "cfg": core}, device_id_type=MESH,
                )
        if order == 0:
            z_in[column(piece, feed.me), 0] = total.astype(jnp.bfloat16)
        else:
            z_out[piece, slot] = total.astype(jnp.bfloat16)
            line_copy(piece, order).start()

    feed.relay(0)
    feed.advance(1)
    if size // 2 < 3:
        second.begin(late)
    feed.ready(0)
    first.own().wait()
    for step in steps:
        first.complete(step)
    second.own().wait()
    expand(0)
    if big:
        if size // 2 >= 3:
            second.begin(late)
        second.pass_on(late)
        for step in steps:
            second.complete(step)
        shrink(0, 0)
    done = 1

    def follow(order):
        feed.relay(order)
        feed.ready(order)
        expand(order)
        if big:
            if order > 1:
                settle(0, order - 2)
            shrink(0, order)
            join(0, order - 1)

    for step in range(2, size // 2 + 1):
        feed.advance(step)
        limit = len(feed.offsets) - (2 if step < size // 2 else 0)
        while done < limit:
            follow(done)
            done += 1
    while done < len(feed.offsets):
        follow(done)
        done += 1
    if big:
        settle(0, size - 2)
        join(0, size - 1)
        settle(0, size - 1)
    else:
        if size // 2 >= 3:
            second.begin(late)
        turns = ([size - 1] + list(range(1, size - 1)) + [0])[-size:]
        waiting = []

        def columns(piece):
            for index, order in enumerate(turns):
                shrink(piece, order)
                if index:
                    join(piece, turns[index - 1])
            join(piece, turns[-1])
            waiting.extend((piece, order) for order in turns)

        def drain(keep):
            while len(waiting) > keep:
                settle(*waiting.pop(0))

        columns(0)
        for piece in range(1, len(early) + 1):
            second.complete(pieces[piece])
            columns(piece)
        for piece in range(len(early) + 1, len(pieces)):
            second.pass_on([pieces[piece]])
        drain(size)
        for piece in range(len(early) + 1, len(pieces)):
            second.complete(pieces[piece])
            columns(piece)
            drain(size)
        drain(0)
    sums = []
    for order in range(1, size):
        for piece in range(groups):
            line_copy(piece, order, True).wait_recv()
    for piece in range(groups):
        total = z_in[piece, 0].astype(jnp.float32)
        for order in range(1, size):
            total = total + z_in[piece, order].astype(jnp.float32)
        sums.append(total[:, :cols])
    feed_out = jnp.concatenate(sums, axis=1)
    ending = res_ref[...] + mod(core, 9) * feed_out
    ending = normed(ending, mod(core, 6), mod(core, 5))
    noise[...] = lax.dot_general(ending, fw_ref[...], flip, preferred_element_type=jnp.float32)
    swap = pltpu.make_async_remote_copy(
        src_ref=noise, dst_ref=noise_in, send_sem=last_s, recv_sem=last_r,
        device_id=partner, device_id_type=MESH,
    )
    swap.start()
    for piece in range(groups):
        for order in range(size):
            if order + depth >= size:
                give_copy(piece, order).wait_send()
                for step in range(1, sides):
                    over_copy(piece, order, step, False).wait_send()
                if order:
                    line_copy(piece, order).wait_send()
    first.end()
    second.end()
    feed.end()
    swap.wait()
    kept = noise[...]
    other = noise_in[...]
    cond = jnp.where(core == 0, kept, other)
    uncond = jnp.where(core == 0, other, kept)
    o_ref[...] = uncond + GUIDANCE * (cond - uncond)


def joint(
    sinusoid_rows, pooled, length, gains, image, words, time_weight, time_second, mod_weight,
    proj_weight, out_weight, expand_weight, reduce_weight, final_weight, head_size, slot_count,
    rows, cut,
):
    axes = ("blk", "ulysses", "cfg")
    count = count_of(axes)
    size = lax.axis_size("blk")
    sides = lax.axis_size("ulysses")
    groups = lax.axis_size("groups")
    branches, _, width = pooled.shape
    inner = proj_weight.shape[2]
    tokens = 2 * rows
    img = sides * tokens
    text = cut - rows
    time_cols = time_second.shape[0]
    mod_cols = mod_weight.shape[0]
    padded = -(-(time_cols + 1) // LANES) * LANES
    quads = sides * 2
    packed = (cut + rows, width)
    all_shape = (quads, size) + packed
    big = 2 * math.prod(all_shape) > 2**24
    parts = groups if expand_weight.shape[0] % (8 * groups) == 0 else 1
    hidden = expand_weight.shape[1]
    piece = window_width(hidden // size, hidden, size)
    peers = pltpu.SemaphoreType.DMA((count,))
    one = pltpu.SemaphoreType.DMA
    some = pltpu.SemaphoreType.DMA((sides,))
    vmem = pl.BlockSpec(memory_space=pltpu.VMEM)
    anywhere = pl.BlockSpec(memory_space=pl.ANY)
    bf16, f32 = jnp.bfloat16, jnp.float32
    depth = 2 if big else size
    pieces = 1 if big else size
    padded_cols = -(-(width // pieces) // LANES) * LANES
    bands = -(-pieces * depth // (width // padded_cols))
    reuse = mod_cols >= bands * img
    inputs = [sinusoid_rows, pooled, length, gains, image, words, final_weight]
    inputs += [time_weight, time_second, mod_weight, proj_weight, out_weight, expand_weight, reduce_weight]
    feed_shape = (quads, size, tokens, width)
    outs = [jax.ShapeDtypeStruct((tokens, final_weight.shape[0]), f32)]
    gathers = [all_shape, feed_shape]
    if big:
        outs += [jax.ShapeDtypeStruct(shape, bf16) for shape in gathers]
    scratch = [] if big else [pltpu.VMEM(shape, bf16) for shape in gathers]
    scratch += [
        pltpu.VMEM(packed, bf16),
        pltpu.VMEM((size * expand_weight.shape[0], piece), bf16),
        pltpu.VMEM((size * reduce_weight.shape[0], piece), bf16),
        pltpu.VMEM((tokens, width), f32),
        pltpu.VMEM((tokens, width), bf16),
        pltpu.VMEM((count, 1, padded), f32),
        pltpu.VMEM((count, branches, mod_cols), f32),
        pltpu.VMEM((branches, 1, count * mod_cols), f32),
        pltpu.VMEM(time_weight.shape, bf16),
        pltpu.VMEM(time_second.shape, bf16),
        pltpu.VMEM(mod_weight.shape, bf16),
        pltpu.VMEM(proj_weight.shape, bf16),
        pltpu.VMEM(out_weight.shape, bf16),
        pltpu.VMEM((quads,) + packed if big else (1, 16, LANES), bf16),
        pltpu.VMEM((2 * img, width), bf16),
        pltpu.VMEM((2 * size * sides, text, width), bf16),
        pltpu.VMEM((2, img, inner), bf16),
        pltpu.VMEM((2, size * img, inner), bf16),
        pltpu.VMEM((2, size * img, inner), bf16),
        pltpu.VMEM((2, size * sides * text, inner), bf16),
        pltpu.VMEM((2, size * sides * text, inner), bf16),
        pltpu.VMEM((img, inner), bf16),
        pltpu.VMEM((img, width), bf16),
        pltpu.VMEM((img, width), bf16),
        pltpu.VMEM((sides, tokens, width), bf16),
        pltpu.VMEM((sides, tokens, width), bf16),
        pltpu.VMEM((16, LANES) if reuse else (depth, img, padded_cols), bf16),
        pltpu.VMEM((pieces, depth, img, padded_cols), bf16),
        pltpu.VMEM((pieces, depth, sides, tokens, padded_cols), bf16),
        pltpu.VMEM((pieces, depth, sides, tokens, padded_cols), bf16),
        pltpu.VMEM((pieces, depth, tokens, padded_cols), bf16),
        pltpu.VMEM((pieces, size, tokens, padded_cols), bf16),
        pltpu.VMEM((tokens, final_weight.shape[0]), f32),
        pltpu.VMEM((tokens, final_weight.shape[0]), f32),
        pltpu.VMEM((1 if big else size, 2 * img, piece), bf16),
        pltpu.SemaphoreType.DMA((5,)),
        peers, peers, peers, peers, one, one, some, some, one,
        pltpu.SemaphoreType.DMA((pieces, depth)),
        pltpu.SemaphoreType.DMA((pieces, depth)),
        pltpu.SemaphoreType.DMA((pieces, depth, sides)),
        pltpu.SemaphoreType.DMA((pieces, depth, sides)),
        pltpu.SemaphoreType.DMA((pieces, depth)),
        pltpu.SemaphoreType.DMA((pieces, size)),
        one, one,
        pltpu.SemaphoreType.REGULAR,
        pltpu.SemaphoreType.REGULAR((sides,)),
    ]
    cfg = dict(
        count=len(inputs) + len(outs) + len(scratch), head_size=head_size, slot_count=slot_count,
        rows=rows, cut=cut, big=big, parts=parts,
        depth=depth, reuse=reuse, groups=pieces,
    )
    return pl.pallas_call(
        functools.partial(joint_kernel, cfg),
        out_shape=outs,
        in_specs=[vmem] * 7 + [anywhere] * 7,
        out_specs=[vmem] + [anywhere] * (len(outs) - 1),
        scratch_shapes=scratch
        + spread_sems()
        + shuffle_sems(parts)
        + shuffle_sems(parts)
        + spread_sems(),
        compiler_params=pltpu.CompilerParams(
            collective_id=0, has_side_effects=True, vmem_limit_bytes=63 * 2**20
        ),
        name="joint",
    )(*inputs)[0]


def body(
    img_tokens,
    text_tokens,
    text_lengths,
    timestep,
    pooled,
    time_weight,
    time_second,
    mod_weight,
    proj_weight,
    out_weight,
    expand_weight,
    reduce_weight,
    qk_gain,
    final_weight,
):
    head_size = qk_gain.shape[1]
    token_count = img_tokens.shape[2]
    slot_count = text_tokens.shape[2]
    rows = token_count // 2
    text_pad = -(-slot_count // 8) * 8
    guided = joint(
        sinusoid(timestep, time_weight.shape[0]).astype(jnp.bfloat16),
        pooled,
        text_lengths.astype(jnp.float32),
        qk_gain,
        img_tokens[0, 0],
        text_tokens[0, 0],
        time_weight,
        time_second.T,
        mod_weight.T,
        proj_weight,
        out_weight,
        expand_weight,
        reduce_weight.T,
        final_weight.T,
        head_size,
        slot_count,
        rows,
        rows + text_pad,
    )
    channels = final_weight.shape[1] // 4
    guided = guided.reshape(token_count, 2, 2, channels)
    kept = lax.dynamic_index_in_dim(guided, lax.axis_index("cfg"), 1, keepdims=False)
    return kept.transpose(2, 0, 1).reshape(1, channels, 1, 2 * token_count)


def solution(mesh):
    in_specs = (
        P("cfg", "groups", ("blk", "ulysses"), None),
        P("cfg", "groups", ("blk", "ulysses"), None),
        P("cfg", "groups"),
        P("groups"),
        P(None, "groups", None),
        P(),
        P(None, ("blk", "ulysses", "cfg")),
        P(None, ("blk", "ulysses", "cfg")),
        P(None, None, ("ulysses", "cfg")),
        P(("ulysses", "cfg"), None),
        P("blk", ("ulysses", "cfg")),
        P(("ulysses", "cfg"), "blk"),
        P(),
        P(),
    )
    out_specs = P("groups", None, ("blk", "ulysses", "cfg"), None)
    return jax.shard_map(body, mesh=mesh, in_specs=in_specs, out_specs=out_specs, check_vma=False)
```

```python
import functools
import math

import jax
import jax.numpy as jnp
from jax import lax
from jax.experimental import pallas as pl
from jax.experimental.pallas import tpu as pltpu
from jax.sharding import PartitionSpec as P

GUIDANCE = 3.5
LN_EPS = 1e-06
RMS_EPS = 1e-06
NEG_FILL = -1e30
LANES = 128
MESH = pl.DeviceIdType.MESH


def sinusoid(timestep, feature_count):
    half_width = feature_count // 2
    frequency = jnp.exp(-math.log(10000.0) * jnp.arange(half_width, dtype=jnp.float32) / half_width)
    angles = timestep.astype(jnp.float32)[:, None] * frequency[None, :]
    return jnp.concatenate([jnp.cos(angles), jnp.sin(angles)], axis=1)


def silu(value):
    return value / (1.0 + jnp.exp(-value))


def flat_position(axes):
    position = 0
    for axis in axes:
        position = position * lax.axis_size(axis) + lax.axis_index(axis)
    return position


def coordinates(position, axes):
    found = {}
    for axis in reversed(axes):
        size = lax.axis_size(axis)
        found[axis] = lax.rem(position, size)
        position = position // size
    return found


def count_of(axes):
    return math.prod(lax.axis_size(axis) for axis in axes)


def normed(values, shift, scale):
    average = jnp.mean(values, axis=-1, keepdims=True)
    centred = values - average
    variance = jnp.mean(centred * centred, axis=-1, keepdims=True)
    return (centred * lax.rsqrt(variance + LN_EPS) * (1.0 + scale) + shift).astype(jnp.bfloat16)


def unit_heads(values, gains, same_head, head_size):
    parts = []
    lanes = same_head.shape[0]
    for first in range(0, values.shape[1], lanes):
        piece = values[:, first : first + lanes]
        square = piece * piece
        high = square.astype(jnp.bfloat16)
        low = (square - high.astype(jnp.float32)).astype(jnp.bfloat16)
        total = jnp.dot(high, same_head, preferred_element_type=jnp.float32)
        total = total + jnp.dot(low, same_head, preferred_element_type=jnp.float32)
        scale = lax.rsqrt(total * (1.0 / head_size) + RMS_EPS)
        parts.append((piece * scale * gains[:, first : first + lanes]).astype(jnp.bfloat16))
    return jnp.concatenate(parts, axis=1)


def window(index, share, total, width):
    start = jnp.minimum(index * share // LANES * LANES, total - width)
    return pl.multiple_of(start, LANES)


def window_width(share, total, parts):
    ends = [-(-(index + 1) * share // LANES) - index * share // LANES for index in range(parts)]
    return min(max(ends) * LANES, total)


class Spread:
    def __init__(self, x_ref, o_ref, sems):
        self.x_ref, self.o_ref = x_ref, o_ref
        self.hop_s, self.hop_r, self.x_s, self.x_r = sems[:4]
        self.c_s, self.c_r, self.f_s, self.f_r = sems[4:8]
        self.local = sems[8]
        self.size = lax.axis_size("blk")
        self.me = lax.axis_index("blk")
        self.sides = lax.axis_size("ulysses")
        self.row = lax.axis_index("ulysses")
        self.core = lax.axis_index("cfg")
        self.partner = {"ulysses": self.row, "cfg": 1 - self.core}
        self.base = o_ref.at[self.row * 2 + self.core]
        self.blocks = [self.me]
        for order in range(1, self.size):
            block = 0
            for place in range(self.size):
                near = sorted(range(self.size), key=lambda other: (abs(other - place), other))
                block = jnp.where(self.me == place, near[order], block)
            self.blocks.append(block)
        self.known = 1
        self.own = pltpu.make_async_copy(x_ref, self.base.at[self.me], self.local)

    def copy(self, source, target, send, recv, device):
        return pltpu.make_async_remote_copy(
            src_ref=source,
            dst_ref=target,
            send_sem=send,
            recv_sem=recv,
            device_id=device,
            device_id_type=MESH,
        )

    def start_own(self, way):
        target = self.base.at[self.me]
        sem = self.size + (way + 1) // 2
        return self.copy(
            self.x_ref, target, self.hop_s.at[sem], self.hop_r.at[self.me],
            {"blk": jnp.clip(self.me + way, 0, self.size - 1)},
        )

    def inside(self, place):
        return jnp.logical_and(place >= 0, place < self.size)

    def onward(self, order):
        block = self.blocks[order]
        target = jnp.where(block < self.me, self.me + 1, self.me - 1)
        copy = self.copy(
            self.base.at[block], self.base.at[block],
            self.hop_s.at[block], self.hop_r.at[block],
            {"blk": jnp.clip(target, 0, self.size - 1)},
        )
        return self.inside(target), copy

    def arriving(self, order):
        block = self.blocks[order]
        source = jnp.where(block < self.me, self.me - 1, self.me + 1)
        return self.copy(
            self.base.at[block], self.base.at[block],
            self.hop_s.at[block], self.hop_r.at[block], {"blk": source},
        )

    def aside(self, step):
        return {"ulysses": lax.rem(self.row + step, self.sides), "cfg": self.core}

    def send(self, order, step):
        slot = self.blocks[order]
        return self.copy(
            self.x_ref if order == 0 else self.base.at[slot],
            self.base.at[slot],
            self.x_s.at[order, step] if step else self.c_s.at[order],
            self.x_r.at[order, step] if step else self.c_r.at[order],
            self.aside(step) if step else self.partner,
        )

    def across_in(self, order, step):
        source = lax.rem(self.row - step + self.sides, self.sides)
        block = self.o_ref.at[source * 2 + self.core, self.blocks[order]]
        return self.copy(
            block, block, self.x_s.at[order, step], self.x_r.at[order, step], self.aside(step)
        )

    def forward(self, order, step, side):
        source = lax.rem(self.row - step + self.sides, self.sides)
        block = self.o_ref.at[source * 2 + side, self.blocks[order]]
        return self.copy(
            block, block, self.f_s.at[order, step], self.f_r.at[order, step], self.partner
        )

    def beside_in(self, order):
        block = self.o_ref.at[self.row * 2 + 1 - self.core, self.blocks[order]]
        return self.copy(block, block, self.c_s.at[order], self.c_r.at[order], self.partner)

    def pass_on(self, order):
        for step in list(range(1, self.sides)) + [0]:
            self.send(order, step).start()

    def begin(self):
        for way in (1, -1):
            pl.when(self.inside(self.me + way))(self.start_own(way).start)
        self.pass_on(0)

    def advance(self, order):
        while self.known <= min(order, self.size - 1):
            self.arriving(self.known).wait_recv()
            needed, copy = self.onward(self.known)
            pl.when(needed)(copy.start)
            self.pass_on(self.known)
            self.known += 1

    def relay(self, order):
        for step in range(1, self.sides):
            self.across_in(order, step).wait_recv()
            self.forward(order, step, self.core).start()

    def ready(self, order):
        for step in range(1, self.sides):
            self.forward(order, step, 1 - self.core).wait_recv()
        self.beside_in(order).wait_recv()
        if order == 0:
            self.own.wait()

    def end(self):
        for way in (1, -1):
            pl.when(self.inside(self.me + way))(self.start_own(way).wait_send)
        for order in range(self.size):
            if order:
                needed, copy = self.onward(order)
                pl.when(needed)(copy.wait_send)
            for step in range(self.sides):
                self.send(order, step).wait_send()
            for step in range(1, self.sides):
                self.forward(order, step, self.core).wait_send()


def spread_sems():
    size = lax.axis_size("blk")
    hops = pltpu.SemaphoreType.DMA((size + 2,))
    across = pltpu.SemaphoreType.DMA((size, lax.axis_size("ulysses")))
    beside = pltpu.SemaphoreType.DMA((size,))
    one = pltpu.SemaphoreType.DMA
    return [hops, hops, across, across, beside, beside, across, across, one]


def greet_all():
    axes = ("blk", "ulysses", "cfg")
    count = count_of(axes)
    place = flat_position(axes)
    groups = lax.axis_size("groups")
    barrier = pltpu.get_barrier_semaphore()

    def greet(step, carry):
        pl.semaphore_signal(
            barrier,
            inc=1,
            device_id=coordinates(lax.rem(place + step, count), axes),
            device_id_type=MESH,
        )
        return carry

    lax.fori_loop(1, count, greet, 0)
    for step in range(1, groups):
        other = lax.rem(lax.axis_index("groups") + step, groups)
        pl.semaphore_signal(barrier, inc=1, device_id={"groups": other}, device_id_type=MESH)
    return barrier, count - 1 + groups - 1


class Shuffle:
    def __init__(self, source, target, sems, parts):
        self.source, self.target, self.parts = source, target, parts
        self.z_s, self.z_r, self.y_s, self.y_r, self.local = sems
        self.size = lax.axis_size("blk")
        self.me = lax.axis_index("blk")
        self.part = lax.axis_index("groups")
        self.rows, self.total = source.shape
        self.share = self.total // self.size
        self.width = target.shape[1]
        self.height = self.rows // parts

    def columns(self, index):
        return pl.ds(window(index, self.share, self.total, self.width), self.width)

    def block(self, index, part):
        start = index * self.rows
        if self.parts > 1:
            start = start + part * self.height
        return self.target.at[pl.ds(pl.multiple_of(start, 8), self.height)]

    def piece(self, index):
        if self.parts == 1:
            return self.source.at[:, self.columns(index)]
        start = pl.multiple_of(self.part * self.height, 8)
        return self.source.at[pl.ds(start, self.height), self.columns(index)]

    def own(self):
        start = pl.multiple_of(self.me * self.rows, 8)
        return pltpu.make_async_copy(
            self.source.at[:, self.columns(self.me)],
            self.target.at[pl.ds(start, self.rows)],
            self.local,
        )

    def remote(self, source, target, send, recv, device):
        return pltpu.make_async_remote_copy(
            src_ref=source,
            dst_ref=target,
            send_sem=send,
            recv_sem=recv,
            device_id=device,
            device_id_type=MESH,
        )

    def out(self, step):
        target = lax.rem(self.me + step, self.size)
        return self.remote(
            self.piece(target),
            self.block(self.me, self.part),
            self.z_s.at[step],
            self.z_r.at[step],
            {"blk": target},
        )

    def into(self, step):
        source = lax.rem(self.me - step + self.size, self.size)
        return self.remote(
            self.block(source, self.part),
            self.block(source, self.part),
            self.z_s.at[step],
            self.z_r.at[step],
            {"blk": source},
        )

    def cross(self, step, turn, arriving):
        origin = lax.rem(self.me - step + self.size, self.size)
        part = self.part
        other = lax.rem(self.part + turn, self.parts)
        if arriving:
            part = other = lax.rem(self.part - turn + self.parts, self.parts)
        block = self.block(origin, part)
        return self.remote(
            block, block, self.y_s.at[step, turn], self.y_r.at[step, turn], {"groups": other}
        )

    def begin(self, steps):
        for step in steps:
            self.out(step).start()

    def order(self):
        half = self.size // 2
        steps = [half] if self.size > 1 else []
        for step in range(1, half + 1):
            steps += [near for near in (half - step, half + step) if 0 < near < self.size]
        return steps

    def pass_on(self, steps):
        for step in steps:
            self.into(step).wait_recv()
            for turn in range(1, self.parts):
                self.cross(step, turn, False).start()

    def complete(self, step):
        for turn in range(1, self.parts):
            self.cross(step, turn, True).wait_recv()

    def end(self):
        for step in self.order():
            self.out(step).wait_send()
            for turn in range(1, self.parts):
                self.cross(step, turn, False).wait_send()


def shuffle_sems(parts):
    size = lax.axis_size("blk")
    line = pltpu.SemaphoreType.DMA((size,))
    grid = pltpu.SemaphoreType.DMA((size, max(parts, 2)))
    return [line, line, grid, grid, pltpu.SemaphoreType.DMA]


def joint_kernel(cfg, *refs):
    (
        sin_ref, pooled_ref, len_ref, gains_ref, img_ref, text_ref,
        fw_ref, tw_hbm, ts_hbm, mw_hbm, pw_hbm, ow_hbm, w1_hbm, w2_hbm,
        o_ref, tok_ref, rows_ref, x_ref, w1_ref, w2_ref, res_ref, feed_ref,
        t_all, m_all, mod_ref, tw_ref, ts_ref, mw_ref, pw_ref, ow_ref,
        stage, h_ref, ht_ref, q_ref, k_ref, v_ref, kt_ref, vt_ref, mix_ref,
        give, got, mine, att, term, gift_in, x_out, x_in, z_out, z_in, noise, noise_in, act_ref,
        load_s, t_s, t_r, m_s, m_r, core_s, core_r, side_s, side_r, stage_s,
        give_s, give_r, over_s, over_r, line_s, line_r, last_s, last_r, free_c, free_x,
    ) = refs[: cfg["count"]]
    sems = list(refs[cfg["count"] :])
    head_size, slot_count = cfg["head_size"], cfg["slot_count"]
    rows, cut, big = cfg["rows"], cfg["cut"], cfg["big"]
    axes = ("blk", "ulysses", "cfg")
    count = count_of(axes)
    place = flat_position(axes)
    size = lax.axis_size("blk")
    sides = lax.axis_size("ulysses")
    row = lax.axis_index("ulysses")
    core = lax.axis_index("cfg")
    width = x_ref.shape[1]
    gain_ref = jnp.concatenate([gains_ref[...]] * (pw_ref.shape[2] // head_size), axis=1)
    inner = pw_ref.shape[2]
    tokens = 2 * rows
    img = sides * tokens
    text = cut - rows
    time_cols = ts_ref.shape[0]
    lanes = 2 * head_size

    loads = [
        pltpu.make_async_copy(source, target, load_s.at[index])
        for index, (source, target) in enumerate(
            [(tw_hbm, tw_ref), (ts_hbm, ts_ref), (mw_hbm, mw_ref), (pw_hbm, pw_ref), (ow_hbm, ow_ref)]
        )
    ]
    for load in loads:
        load.start()
    spread = Spread(x_ref, tok_ref, sems[:9])
    first = Shuffle(w1_hbm, w1_ref, sems[9:14], cfg["parts"])
    second = Shuffle(w2_hbm, w2_ref, sems[14:19], cfg["parts"])
    feed = Spread(feed_ref, rows_ref, sems[19:28])
    if cfg["reuse"]:
        term = mw_ref
    barrier, expected = greet_all()
    x_ref[:rows] = img_ref[:rows]
    x_ref[cut:] = img_ref[rows:]
    words = [text_ref[...]]
    if text > slot_count:
        words.append(jnp.zeros((text - slot_count, width), jnp.bfloat16))
    x_ref[rows:cut] = jnp.concatenate(words, axis=0)

    def outgoing(ref, send, recv, step):
        return pltpu.make_async_remote_copy(
            src_ref=ref.at[place],
            dst_ref=ref.at[place],
            send_sem=send.at[step],
            recv_sem=recv.at[step],
            device_id=coordinates(lax.rem(place + step, count), axes),
            device_id_type=MESH,
        )

    def incoming(ref, send, recv, step):
        source = lax.rem(place - step + count, count)
        return pltpu.make_async_remote_copy(
            src_ref=ref.at[source],
            dst_ref=ref.at[source],
            send_sem=send.at[step],
            recv_sem=recv.at[step],
            device_id=coordinates(source, axes),
            device_id_type=MESH,
        )

    def send_all(ref, send, recv):
        def begin(step, carry):
            outgoing(ref, send, recv, step).start()
            return carry

        lax.fori_loop(1, count, begin, 0)

    def wait_all(ref, send, recv):
        def finish(step, carry):
            incoming(ref, send, recv, step).wait_recv()
            outgoing(ref, send, recv, step).wait_send()
            return carry

        lax.fori_loop(1, count, finish, 0)

    flip = (((1,), (1,)), ((), ()))
    loads[0].wait()
    sin_rows = jnp.broadcast_to(sin_ref[...], (16, sin_ref.shape[1]))
    hidden = jnp.dot(sin_rows, tw_ref[...], preferred_element_type=jnp.float32)
    hidden = silu(hidden).astype(jnp.bfloat16)
    loads[1].wait()
    part = lax.dot_general(hidden, ts_ref[...], flip, preferred_element_type=jnp.float32)[0:1]
    length = jnp.broadcast_to(len_ref[...], (1, t_all.shape[2] - time_cols))
    t_all[place] = jnp.concatenate([part, length], axis=1)
    pl.semaphore_wait(barrier, expected)
    send_all(t_all, t_s, t_r)
    spread.own.start()
    spread.begin()
    wait_all(t_all, t_s, t_r)
    embed = jnp.concatenate([t_all[i][:, :time_cols] for i in range(count)], axis=1)
    acted = [silu(embed + pooled_ref[branch]) for branch in range(2)]
    acted = jnp.concatenate(acted + [jnp.zeros((14, width), jnp.float32)], axis=0)
    acted = acted.astype(jnp.bfloat16)
    loads[2].wait()
    mods = lax.dot_general(acted, mw_ref[...], flip, preferred_element_type=jnp.float32)
    m_all[place] = mods[0:2]
    send_all(m_all, m_s, m_r)
    spread.advance(1)
    spread.relay(0)
    wait_all(m_all, m_s, m_r)
    for branch in range(2):
        mod_ref[branch] = jnp.concatenate(
            [m_all[i][branch : branch + 1] for i in range(count)], axis=1
        )

    def mod(branch, index):
        return mod_ref[branch, :, index * width : (index + 1) * width]

    head_row = lax.broadcasted_iota(jnp.int32, (lanes, lanes), 0) // head_size
    head_col = lax.broadcasted_iota(jnp.int32, (lanes, lanes), 1) // head_size
    same_head = jnp.where(head_row == head_col, 1.0, 0.0).astype(jnp.bfloat16)

    steps = first.order()
    early = steps[: (len(steps) + 2) // 3]
    late = steps[len(early) :]

    def start_weights():
        first.own().start()
        second.own().start()
        first.begin(steps)
        second.begin(early)

    def project(order):
        slot = spread.blocks[order]
        if big:
            fetch = pltpu.make_async_copy(tok_ref.at[:, slot], stage, stage_s)
            fetch.start()
            fetch.wait()

        def tile(side, branch):
            index = side * 2 + branch
            return stage[index] if big else tok_ref[index, slot]

        for branch in range(2):
            for side in range(sides):
                x = tile(side, branch).astype(jnp.float32)
                start = branch * img + side * tokens
                h_ref[start : start + rows] = normed(x[:rows], mod(branch, 0), mod(branch, 1))
                h_ref[start + rows : start + tokens] = normed(
                    x[cut:], mod(branch, 0), mod(branch, 1)
                )
                spot = (branch * size + order) * sides + side
                ht_ref[spot] = normed(x[rows:cut], mod(branch, 4), mod(branch, 3))
        keys = jnp.dot(h_ref[...], pw_ref[1], preferred_element_type=jnp.float32)
        keys = unit_heads(keys, gain_ref[1:2], same_head, head_size)
        values = jnp.dot(h_ref[...], pw_ref[2], preferred_element_type=jnp.float32)
        values = values.astype(jnp.bfloat16)
        for branch in range(2):
            here = slice(branch * img, (branch + 1) * img)
            k_ref[branch, order * img : (order + 1) * img] = keys[here]
            v_ref[branch, order * img : (order + 1) * img] = values[here]
        if order == 0:
            found = jnp.dot(h_ref[...], pw_ref[0], preferred_element_type=jnp.float32)
            found = unit_heads(found, gain_ref[0:1], same_head, head_size)
            found = found * jnp.asarray(1.0 / math.sqrt(head_size), jnp.bfloat16)
            for branch in range(2):
                q_ref[branch] = found[branch * img : (branch + 1) * img]

    spread.advance(2)
    spread.ready(0)
    loads[3].wait()
    project(0)
    spread.advance(size)
    start_weights()
    for order in range(1, size):
        spread.relay(order)
        spread.ready(order)
        project(order)

    texts = ht_ref[...].reshape(-1, width)
    keys = jnp.dot(texts, pw_ref[3], preferred_element_type=jnp.float32)
    keys = unit_heads(keys, gain_ref[2:3], same_head, head_size)
    values = jnp.dot(texts, pw_ref[4], preferred_element_type=jnp.float32).astype(jnp.bfloat16)
    slots = size * sides * text
    for branch in range(2):
        kt_ref[branch] = keys[branch * slots : (branch + 1) * slots]
        vt_ref[branch] = values[branch * slots : (branch + 1) * slots]
    spot = lax.broadcasted_iota(jnp.int32, (1, slots), 1)
    within = lax.rem(spot, text)
    side_of = lax.rem(spot // text, sides)
    order_of = spot // (text * sides)
    block_of = jnp.zeros_like(spot)
    for order, block in enumerate(spread.blocks):
        block_of = jnp.where(order_of == order, block, block_of)
    slot_of = (block_of * sides + side_of) * slot_count + within
    chunk = img
    while chunk % 32 == 0 and 8 * chunk * k_ref.shape[1] > 2**20:
        chunk //= 2
    low = lax.broadcasted_iota(jnp.int32, (1, lanes), 1) < head_size
    loads[4].wait()
    partner = {"ulysses": row, "cfg": 1 - core}
    gift = pltpu.make_async_remote_copy(
        src_ref=give, dst_ref=got, send_sem=core_s, recv_sem=core_r,
        device_id=partner, device_id_type=MESH,
    )
    for turn in range(2):
        branch = 1 - core if turn == 0 else core
        limit = t_all[branch][:, time_cols : time_cols + 1].astype(jnp.int32)
        live = jnp.logical_and(slot_of < limit, within < slot_count)
        for left in range(0, inner, lanes):
            here = slice(left, left + lanes)

            def attend(step, carry, branch=branch, here=here, live=live):
                begin = step * chunk
                if chunk < img:
                    begin = pl.multiple_of(begin, chunk)
                queries = q_ref[branch, pl.ds(begin, chunk), here]
                nothing = jnp.zeros_like(queries)
                pair = jnp.concatenate(
                    [jnp.where(low, queries, nothing), jnp.where(low, nothing, queries)], axis=0
                )
                scores = lax.dot_general(
                    pair, k_ref[branch, :, here], flip, preferred_element_type=jnp.float32
                )
                words = lax.dot_general(
                    pair, kt_ref[branch, :, here], flip, preferred_element_type=jnp.float32
                )
                words = jnp.where(live, words, NEG_FILL)
                largest = jnp.maximum(
                    jnp.max(scores, axis=1, keepdims=True), jnp.max(words, axis=1, keepdims=True)
                )
                scores = jnp.exp(scores - largest)
                words = jnp.exp(words - largest)
                denominator = jnp.sum(scores, axis=1, keepdims=True)
                denominator = denominator + jnp.sum(words, axis=1, keepdims=True)
                update = jnp.dot(
                    scores.astype(jnp.bfloat16),
                    v_ref[branch, :, here],
                    preferred_element_type=jnp.float32,
                )
                update = update + jnp.dot(
                    words.astype(jnp.bfloat16),
                    vt_ref[branch, :, here],
                    preferred_element_type=jnp.float32,
                )
                update = update / denominator
                both = jnp.where(low, update[:chunk], update[chunk:]).astype(jnp.bfloat16)
                mix_ref[pl.ds(begin, chunk), here] = both
                return carry

            if chunk == img:
                attend(0, 0)
            else:
                lax.fori_loop(0, img // chunk, attend, 0)
        if turn == 0:
            out = jnp.dot(mix_ref[...], ow_ref[...], preferred_element_type=jnp.float32)
            give[...] = out.astype(jnp.bfloat16)
            gift.start()

    def aside(step):
        return {"ulysses": lax.rem(row + step, sides), "cfg": core}

    def to_side(step):
        side = lax.rem(row + step, sides)
        return pltpu.make_async_remote_copy(
            src_ref=mine.at[side], dst_ref=att.at[row],
            send_sem=side_s.at[step], recv_sem=side_r.at[step],
            device_id=aside(step), device_id_type=MESH,
        )

    def from_side(step):
        side = lax.rem(row - step + sides, sides)
        return pltpu.make_async_remote_copy(
            src_ref=mine.at[side], dst_ref=att.at[side],
            send_sem=side_s.at[step], recv_sem=side_r.at[step],
            device_id=aside(step), device_id_type=MESH,
        )

    for step in list(range(1, sides)) + [0]:
        side = lax.rem(row + step, sides)
        start = pl.multiple_of(side * tokens, tokens)
        out = jnp.dot(
            mix_ref[pl.ds(start, tokens)], ow_ref[...], preferred_element_type=jnp.float32
        )
        if step == (1 if sides > 1 else 0):
            gift.wait_recv()
        out = out.astype(jnp.bfloat16).astype(jnp.float32)
        total = out + got[pl.ds(start, tokens)].astype(jnp.float32)
        if step:
            mine[side] = total.astype(jnp.bfloat16)
            to_side(step).start()
        else:
            att[row] = total.astype(jnp.bfloat16)
    for step in range(1, sides):
        from_side(step).wait_recv()
    own_x = img_ref[...].astype(jnp.float32)
    attended = att[0].astype(jnp.float32)
    for side in range(1, sides):
        attended = attended + att[side].astype(jnp.float32)
    residual = own_x + mod(core, 2) * attended
    res_ref[...] = residual
    feed_ref[...] = normed(residual, mod(core, 7), mod(core, 8))
    feed.own.start()
    feed.begin()
    first.pass_on(steps)
    second.pass_on(early)
    gift.wait_send()
    for step in range(1, sides):
        to_side(step).wait_send()
    spread.end()

    depth, groups = cfg["depth"], cfg["groups"]
    span = sides * tokens
    cols = width // groups
    padded = z_in.shape[3]
    hidden = w1_ref.shape[1]
    share = w1_hbm.shape[1] // size
    begins = window(lax.axis_index("blk"), share, w1_hbm.shape[1], hidden)
    lane = begins + lax.broadcasted_iota(jnp.int32, (1, hidden), 1)
    base = lax.axis_index("blk") * share
    owned = jnp.logical_and(lane >= base, lane < base + share)
    pieces = [0] + steps

    def column(piece, source):
        return lax.rem(source - pieces[piece] + size, size) if groups > 1 else 0

    def term_at(piece, slot):
        if not cfg["reuse"]:
            return term.at[slot]
        unit = piece * depth + slot
        strips = width // padded
        return term.at[
            pl.ds(unit // strips * span, span), pl.ds(unit % strips * padded, padded)
        ]

    def give_copy(piece, order):
        slot = order % depth
        return pltpu.make_async_remote_copy(
            src_ref=term_at(piece, slot), dst_ref=gift_in.at[piece, slot],
            send_sem=give_s.at[piece, slot], recv_sem=give_r.at[piece, slot],
            device_id=partner, device_id_type=MESH,
        )

    def over_copy(piece, order, step, arriving):
        slot = order % depth
        side = lax.rem(row + step, sides)
        source = row
        if arriving:
            side = source = lax.rem(row - step + sides, sides)
        return pltpu.make_async_remote_copy(
            src_ref=x_out.at[piece, slot, side], dst_ref=x_in.at[piece, slot, source],
            send_sem=over_s.at[piece, slot, step], recv_sem=over_r.at[piece, slot, step],
            device_id=aside(step), device_id_type=MESH,
        )

    def line_copy(piece, order, arriving=False):
        slot = order % depth
        other = feed.blocks[order]
        source = other if arriving else feed.me
        return pltpu.make_async_remote_copy(
            src_ref=z_out.at[piece, slot], dst_ref=z_in.at[column(piece, source), source],
            send_sem=line_s.at[piece, slot], recv_sem=line_r.at[piece, source],
            device_id={"blk": other}, device_id_type=MESH,
        )

    def expand(order):
        where = feed.blocks[order]
        if big:
            fetch = pltpu.make_async_copy(
                rows_ref.at[:, where], stage.at[:, pl.ds(0, tokens)], stage_s
            )
            fetch.start()
            fetch.wait()

        def rows_of(index):
            return stage[index, :tokens] if big else rows_ref[index, where]

        block = [rows_of(side * 2 + core) for side in range(sides)]
        block += [rows_of(side * 2 + 1 - core) for side in range(sides)]
        block = jnp.concatenate(block, axis=0)
        pre = jnp.dot(block, w1_ref[...], preferred_element_type=jnp.float32)
        act = jnp.where(owned, jax.nn.gelu(pre, approximate=True), 0.0)
        act_ref[0 if big else order] = act.astype(jnp.bfloat16)

    def shrink(piece, order):
        slot = order % depth
        if order >= depth:
            give_copy(piece, order - depth).wait_send()
            for step in range(1, sides):
                over_copy(piece, order - depth, step, False).wait_send()
            pl.semaphore_wait(free_c, 1)
        act = act_ref[0 if big else order]
        if groups > 1:
            start = pl.multiple_of(column(piece, feed.me) * cols, 8)
            weight = w2_ref[pl.ds(start, cols)]
        else:
            weight = w2_ref[...]
        out = lax.dot_general(act, weight, flip, preferred_element_type=jnp.float32)
        if padded > cols:
            out = jnp.concatenate(
                [out, jnp.zeros((out.shape[0], padded - cols), jnp.float32)], axis=1
            )
        out = out.astype(jnp.bfloat16)
        if cfg["reuse"]:
            unit = piece * depth + slot
            strips = width // padded
            high, left = unit // strips * span, unit % strips * padded
            term[high : high + span, left : left + padded] = out[span:]
        else:
            term[slot] = out[span:]
        give_copy(piece, order).start()
        for side in range(sides):
            x_out[piece, slot, side] = out[side * tokens : (side + 1) * tokens]

    def join(piece, order):
        slot = order % depth
        if order >= depth:
            for step in range(1, sides):
                pl.semaphore_wait(free_x.at[step], 1)
        give_copy(piece, order).wait_recv()
        for step in list(range(1, sides)) + [0]:
            side = lax.rem(row + step, sides)
            near = pl.multiple_of(side * tokens, tokens)
            total = x_out[piece, slot, side].astype(jnp.float32)
            total = total + gift_in[piece, slot, pl.ds(near, tokens)].astype(jnp.float32)
            x_out[piece, slot, side] = total.astype(jnp.bfloat16)
            if step:
                over_copy(piece, order, step, False).start()
        if order + depth < size:
            pl.semaphore_signal(free_c, inc=1, device_id=partner, device_id_type=MESH)

    def settle(piece, order):
        slot = order % depth
        if order > depth:
            line_copy(piece, order - depth).wait_send()
        total = x_out[piece, slot, row].astype(jnp.float32)
        for step in range(1, sides):
            over_copy(piece, order, step, True).wait_recv()
            source = lax.rem(row - step + sides, sides)
            total = total + x_in[piece, slot, source].astype(jnp.float32)
            if order + depth < size:
                pl.semaphore_signal(
                    free_x.at[step], inc=1,
                    device_id={"ulysses": source, "cfg": core}, device_id_type=MESH,
                )
        if order == 0:
            z_in[column(piece, feed.me), feed.me] = total.astype(jnp.bfloat16)
        else:
            z_out[piece, slot] = total.astype(jnp.bfloat16)
            line_copy(piece, order).start()

    feed.relay(0)
    feed.advance(size)
    second.begin(late)
    feed.ready(0)
    first.own().wait()
    for step in steps:
        first.complete(step)
    second.own().wait()
    expand(0)
    if big:
        second.pass_on(late)
        for step in steps:
            second.complete(step)
        shrink(0, 0)

    def follow(order):
        feed.relay(order)
        feed.ready(order)
        expand(order)
        if big:
            if order > 1:
                settle(0, order - 2)
            shrink(0, order)
            join(0, order - 1)

    for order in range(1, size):
        follow(order)
    if big:
        settle(0, size - 2)
        join(0, size - 1)
        settle(0, size - 1)
    else:
        turns = ([size - 1] + list(range(1, size - 1)) + [0])[-size:]
        waiting = []

        def columns(piece):
            for index, order in enumerate(turns):
                shrink(piece, order)
                if index:
                    join(piece, turns[index - 1])
            join(piece, turns[-1])
            waiting.extend((piece, order) for order in turns)

        def drain(keep):
            while len(waiting) > keep:
                settle(*waiting.pop(0))

        columns(0)
        for piece in range(1, len(early) + 1):
            second.complete(pieces[piece])
            columns(piece)
        for piece in range(len(early) + 1, len(pieces)):
            second.pass_on([pieces[piece]])
        drain(size)
        for piece in range(len(early) + 1, len(pieces)):
            second.complete(pieces[piece])
            columns(piece)
            drain(size)
        drain(0)
    sums = []
    for order in range(1, size):
        for piece in range(groups):
            line_copy(piece, order, True).wait_recv()
    for piece in range(groups):
        total = z_in[piece, 0].astype(jnp.float32)
        for order in range(1, size):
            total = total + z_in[piece, order].astype(jnp.float32)
        sums.append(total[:, :cols])
    feed_out = jnp.concatenate(sums, axis=1)
    ending = res_ref[...] + mod(core, 9) * feed_out
    ending = normed(ending, mod(core, 6), mod(core, 5))
    noise[...] = lax.dot_general(ending, fw_ref[...], flip, preferred_element_type=jnp.float32)
    swap = pltpu.make_async_remote_copy(
        src_ref=noise, dst_ref=noise_in, send_sem=last_s, recv_sem=last_r,
        device_id=partner, device_id_type=MESH,
    )
    swap.start()
    for piece in range(groups):
        for order in range(size):
            if order + depth >= size:
                give_copy(piece, order).wait_send()
                for step in range(1, sides):
                    over_copy(piece, order, step, False).wait_send()
                if order:
                    line_copy(piece, order).wait_send()
    first.end()
    second.end()
    feed.end()
    swap.wait()
    kept = noise[...]
    other = noise_in[...]
    cond = jnp.where(core == 0, kept, other)
    uncond = jnp.where(core == 0, other, kept)
    o_ref[...] = uncond + GUIDANCE * (cond - uncond)


def joint(
    sinusoid_rows, pooled, length, gains, image, words, time_weight, time_second, mod_weight,
    proj_weight, out_weight, expand_weight, reduce_weight, final_weight, head_size, slot_count,
    rows, cut,
):
    axes = ("blk", "ulysses", "cfg")
    count = count_of(axes)
    size = lax.axis_size("blk")
    sides = lax.axis_size("ulysses")
    groups = lax.axis_size("groups")
    branches, _, width = pooled.shape
    inner = proj_weight.shape[2]
    tokens = 2 * rows
    img = sides * tokens
    text = cut - rows
    time_cols = time_second.shape[0]
    mod_cols = mod_weight.shape[0]
    padded = -(-(time_cols + 1) // LANES) * LANES
    quads = sides * 2
    packed = (cut + rows, width)
    all_shape = (quads, size) + packed
    big = 2 * math.prod(all_shape) > 2**24
    parts = groups if expand_weight.shape[0] % (8 * groups) == 0 else 1
    hidden = expand_weight.shape[1]
    piece = window_width(hidden // size, hidden, size)
    peers = pltpu.SemaphoreType.DMA((count,))
    one = pltpu.SemaphoreType.DMA
    some = pltpu.SemaphoreType.DMA((sides,))
    vmem = pl.BlockSpec(memory_space=pltpu.VMEM)
    anywhere = pl.BlockSpec(memory_space=pl.ANY)
    bf16, f32 = jnp.bfloat16, jnp.float32
    depth = 2 if big else size
    pieces = 1 if big else size
    padded_cols = -(-(width // pieces) // LANES) * LANES
    bands = -(-pieces * depth // (width // padded_cols))
    reuse = mod_cols >= bands * img
    inputs = [sinusoid_rows, pooled, length, gains, image, words, final_weight]
    inputs += [time_weight, time_second, mod_weight, proj_weight, out_weight, expand_weight, reduce_weight]
    feed_shape = (quads, size, tokens, width)
    outs = [jax.ShapeDtypeStruct((tokens, final_weight.shape[0]), f32)]
    gathers = [all_shape, feed_shape]
    if big:
        outs += [jax.ShapeDtypeStruct(shape, bf16) for shape in gathers]
    scratch = [] if big else [pltpu.VMEM(shape, bf16) for shape in gathers]
    scratch += [
        pltpu.VMEM(packed, bf16),
        pltpu.VMEM((size * expand_weight.shape[0], piece), bf16),
        pltpu.VMEM((size * reduce_weight.shape[0], piece), bf16),
        pltpu.VMEM((tokens, width), f32),
        pltpu.VMEM((tokens, width), bf16),
        pltpu.VMEM((count, 1, padded), f32),
        pltpu.VMEM((count, branches, mod_cols), f32),
        pltpu.VMEM((branches, 1, count * mod_cols), f32),
        pltpu.VMEM(time_weight.shape, bf16),
        pltpu.VMEM(time_second.shape, bf16),
        pltpu.VMEM(mod_weight.shape, bf16),
        pltpu.VMEM(proj_weight.shape, bf16),
        pltpu.VMEM(out_weight.shape, bf16),
        pltpu.VMEM((quads,) + packed if big else (1, 16, LANES), bf16),
        pltpu.VMEM((2 * img, width), bf16),
        pltpu.VMEM((2 * size * sides, text, width), bf16),
        pltpu.VMEM((2, img, inner), bf16),
        pltpu.VMEM((2, size * img, inner), bf16),
        pltpu.VMEM((2, size * img, inner), bf16),
        pltpu.VMEM((2, size * sides * text, inner), bf16),
        pltpu.VMEM((2, size * sides * text, inner), bf16),
        pltpu.VMEM((img, inner), bf16),
        pltpu.VMEM((img, width), bf16),
        pltpu.VMEM((img, width), bf16),
        pltpu.VMEM((sides, tokens, width), bf16),
        pltpu.VMEM((sides, tokens, width), bf16),
        pltpu.VMEM((16, LANES) if reuse else (depth, img, padded_cols), bf16),
        pltpu.VMEM((pieces, depth, img, padded_cols), bf16),
        pltpu.VMEM((pieces, depth, sides, tokens, padded_cols), bf16),
        pltpu.VMEM((pieces, depth, sides, tokens, padded_cols), bf16),
        pltpu.VMEM((pieces, depth, tokens, padded_cols), bf16),
        pltpu.VMEM((pieces, size, tokens, padded_cols), bf16),
        pltpu.VMEM((tokens, final_weight.shape[0]), f32),
        pltpu.VMEM((tokens, final_weight.shape[0]), f32),
        pltpu.VMEM((1 if big else size, 2 * img, piece), bf16),
        pltpu.SemaphoreType.DMA((5,)),
        peers, peers, peers, peers, one, one, some, some, one,
        pltpu.SemaphoreType.DMA((pieces, depth)),
        pltpu.SemaphoreType.DMA((pieces, depth)),
        pltpu.SemaphoreType.DMA((pieces, depth, sides)),
        pltpu.SemaphoreType.DMA((pieces, depth, sides)),
        pltpu.SemaphoreType.DMA((pieces, depth)),
        pltpu.SemaphoreType.DMA((pieces, size)),
        one, one,
        pltpu.SemaphoreType.REGULAR,
        pltpu.SemaphoreType.REGULAR((sides,)),
    ]
    cfg = dict(
        count=len(inputs) + len(outs) + len(scratch), head_size=head_size, slot_count=slot_count,
        rows=rows, cut=cut, big=big, parts=parts,
        depth=depth, reuse=reuse, groups=pieces,
    )
    return pl.pallas_call(
        functools.partial(joint_kernel, cfg),
        out_shape=outs,
        in_specs=[vmem] * 7 + [anywhere] * 7,
        out_specs=[vmem] + [anywhere] * (len(outs) - 1),
        scratch_shapes=scratch
        + spread_sems()
        + shuffle_sems(parts)
        + shuffle_sems(parts)
        + spread_sems(),
        compiler_params=pltpu.CompilerParams(
            collective_id=0, has_side_effects=True, vmem_limit_bytes=63 * 2**20
        ),
        name="joint",
    )(*inputs)[0]


def body(
    img_tokens,
    text_tokens,
    text_lengths,
    timestep,
    pooled,
    time_weight,
    time_second,
    mod_weight,
    proj_weight,
    out_weight,
    expand_weight,
    reduce_weight,
    qk_gain,
    final_weight,
):
    head_size = qk_gain.shape[1]
    token_count = img_tokens.shape[2]
    slot_count = text_tokens.shape[2]
    rows = token_count // 2
    text_pad = -(-slot_count // 8) * 8
    guided = joint(
        sinusoid(timestep, time_weight.shape[0]).astype(jnp.bfloat16),
        pooled,
        text_lengths.astype(jnp.float32),
        qk_gain,
        img_tokens[0, 0],
        text_tokens[0, 0],
        time_weight,
        time_second.T,
        mod_weight.T,
        proj_weight,
        out_weight,
        expand_weight,
        reduce_weight.T,
        final_weight.T,
        head_size,
        slot_count,
        rows,
        rows + text_pad,
    )
    channels = final_weight.shape[1] // 4
    guided = guided.reshape(token_count, 2, 2, channels)
    kept = lax.dynamic_index_in_dim(guided, lax.axis_index("cfg"), 1, keepdims=False)
    return kept.transpose(2, 0, 1).reshape(1, channels, 1, 2 * token_count)


def solution(mesh):
    in_specs = (
        P("cfg", "groups", ("blk", "ulysses"), None),
        P("cfg", "groups", ("blk", "ulysses"), None),
        P("cfg", "groups"),
        P("groups"),
        P(None, "groups", None),
        P(),
        P(None, ("blk", "ulysses", "cfg")),
        P(None, ("blk", "ulysses", "cfg")),
        P(None, None, ("ulysses", "cfg")),
        P(("ulysses", "cfg"), None),
        P("blk", ("ulysses", "cfg")),
        P(("ulysses", "cfg"), "blk"),
        P(),
        P(),
    )
    out_specs = P("groups", None, ("blk", "ulysses", "cfg"), None)
    return jax.shard_map(body, mesh=mesh, in_specs=in_specs, out_specs=out_specs, check_vma=False)
```
